256 devices in a mesh: gx: 8 (over z), gy: 4 (over y), gz: 8 (over x, core).
Axes of the slice: x: 4, y: 4, z: 8, core: 2. Of those that a mesh axis runs over, the one named last changes fastest.
Arguments:
- field: bfloat16 [32, 64, 32, 1024], P(None, 'gx', 'gy', 'gz'), may hold values from -6 to 6
- mixing: bfloat16 [32, 32], replicated, may hold values from -1 to 1
- kernel_fine: bfloat16 [3, 3, 3, 32, 32], replicated, may hold values from -0.21875 to 0.21875
- kernel_half: bfloat16 [3, 3, 3, 32, 32], replicated, may hold values from -1.5 to 1.5
- kernel_quarter: bfloat16 [3, 3, 3, 32, 32], replicated, may hold values from -4 to 4
- kernel_eighth: bfloat16 [3, 3, 3, 32, 32], replicated, may hold values from -6 to 6
Outputs:
- layer_out: bfloat16 [32, 64, 32, 1024], P(None, 'gx', 'gy', 'gz')
The draws below stay inside these ranges and needn't reach their ends.
All inputs are finite; a program needn't handle non-finite values.
Results may differ from the reference program's by a relative error of at most 0.008.
Values may be sent and summed in bfloat16 or wider, within the bound.
No kernel may reach another device: no remote copies, remote signals or barrier semaphores. Data moves between devices by JAX's collectives and lax.ppermute only.
A program may use at most 128 MiB of HBM per device.

```python
import jax
import jax.numpy as jnp
from jax import lax

C = 32
NX = 64
NY = 32
NZ = 1024


def level_of(rng, shape, shards, low, largest):
    def one(dim, blocks):
        draws = jax.random.uniform(jax.random.fold_in(jax.random.fold_in(rng, 6), dim), (blocks,), jnp.float32, low / len(shards), largest / len(shards))
        return jnp.repeat(jnp.exp(draws), shape[dim] // blocks).reshape((-1,) + (1,) * (len(shape) - dim - 1))

    factor_of = one(*shards[0])
    for cut in shards[1:]:
        factor_of = factor_of * one(*cut)
    return factor_of


def noise(own_key, dims, deviation, bound, pieces=(), held_as=jnp.bfloat16):
    level = level_of(own_key, dims, pieces, -0.22, 0.18) if pieces else 1.0
    drawn = jax.random.normal(own_key, dims, jnp.float32) * deviation * level
    return jnp.minimum(jnp.maximum(drawn, -bound), bound).astype(held_as)


def setup_inputs(seed: int = 0) -> dict:
    seeds = jax.random.split(jax.random.key(seed), 7)
    field = noise(seeds[0], (C, NX, NY, NZ), 1.0, 6.0, ((1, 8), (2, 4), (3, 8)))
    mixing = noise(seeds[1], (C, C), C ** -0.5, 1.0)
    kernel_fine = noise(seeds[2], (3, 3, 3, C, C), (27 * C) ** -0.5, 0.21875)
    kernel_half = noise(seeds[3], (3, 3, 3, C, C), (3 * (27 * C) ** -0.5), 1.5)
    kernel_quarter = noise(seeds[4], (3, 3, 3, C, C), (9 * (27 * C) ** -0.5), 4.0)
    kernel_eighth = noise(seeds[5], (3, 3, 3, C, C), (27 * (27 * C) ** -0.5), 6.0)
    return dict(field=field, mixing=mixing, kernel_fine=kernel_fine, kernel_half=kernel_half, kernel_quarter=kernel_quarter, kernel_eighth=kernel_eighth)


def restrict(values):
    chans, sizex, sizey, sizez = values.shape
    blocks = values.astype(jnp.float32).reshape(chans, sizex // 2, 2, sizey // 2, 2, sizez // 2, 2)
    return jnp.mean(blocks, axis=(2, 4, 6)).astype(jnp.bfloat16)


def kernel_apply(values, kernel):
    result = lax.conv_general_dilated(values[None], kernel, (1, 1, 1), ((1, 1), (1, 1), (1, 1)),
                                      dimension_numbers=("NCDHW", "DHWIO", "NCDHW"),
                                      preferred_element_type=jnp.float32)
    return result[0]


def refine_padded(padded, dimension):
    length = padded.shape[dimension]
    inner = lax.slice_in_dim(padded, 1, length - 1, axis=dimension)
    lower = lax.slice_in_dim(padded, 0, length - 2, axis=dimension)
    upper = lax.slice_in_dim(padded, 2, length, axis=dimension)
    even_cells = 0.75 * inner + 0.25 * lower
    odd_cells = 0.75 * inner + 0.25 * upper
    joined = jnp.stack([even_cells, odd_cells], axis=dimension + 1)
    shape_out = list(inner.shape)
    shape_out[dimension] = shape_out[dimension] * 2
    return joined.reshape(shape_out)


def prolong(values):
    current = values.astype(jnp.float32)
    for dimension in (1, 2, 3):
        widths = [(0, 0)] * 4
        widths[dimension] = (1, 1)
        current = refine_padded(jnp.pad(current, widths), dimension)
    return current


def reference(field, mixing, kernel_fine, kernel_half, kernel_quarter, kernel_eighth):
    kernels = (kernel_fine, kernel_half, kernel_quarter, kernel_eighth)
    levels_list = [field]
    for depth in range(3):
        levels_list.append(restrict(levels_list[-1]))
    outputs = [kernel_apply(levels_list[depth], kernels[depth]) for depth in range(4)]
    carried = outputs[3].astype(jnp.bfloat16)
    for depth in (2, 1):
        carried = (outputs[depth] + prolong(carried)).astype(jnp.bfloat16)
    chans = field.shape[0]
    mixed = jnp.dot(mixing, field.reshape(chans, -1), preferred_element_type=jnp.float32).reshape(field.shape)
    total = mixed + outputs[0] + prolong(carried)
    return jax.nn.gelu(total, approximate=True).astype(jnp.bfloat16)
```

```python
import jax
import jax.numpy as jnp
import numpy as np
from jax import lax
from jax.experimental import pallas as pl
from jax.experimental.pallas import tpu as pltpu
from jax.sharding import PartitionSpec as P

INTERPRET = False
F32, BF16 = jnp.float32, jnp.bfloat16
LANES = 128


def tables():
    r1 = np.zeros((512, 128), np.float32)
    r2 = np.zeros((512, 128), np.float32)
    r3 = np.zeros((512, 384), np.float32)
    for s in range(4):
        base = s * 128
        for z in range(128):
            r1[base + z, 2 + z // 2] = 0.125
        r1[base, 72 + s] = 1.0
        r1[base + 127, 76 + s] = 1.0
        for z in range(64):
            r2[base + 2 + z, 2 + z // 2] = 0.125
        for k, lane in enumerate((2, 3, 72, 73, 74, 75)):
            r2[base + lane, 40 + 6 * s + k] = 1.0
        for k, lane in enumerate((76, 77, 78, 79, 64, 65)):
            r2[base + lane, 64 + 6 * s + k] = 1.0
        for z in range(32):
            r3[base + 2 + z, 2 + z // 2] = 0.125
        for sub in range(4):
            tile = (2 * (s // 2) + sub // 2) * 4 + 2 * (s % 2) + sub % 2
            for k in range(6):
                r3[base + 40 + 6 * sub + k, 128 + 6 * tile + k] = 1.0
                r3[base + 64 + 6 * sub + k, 256 + 6 * tile + k] = 1.0
        for k in range(2):
            r3[base + 2 + k, 128 + 96 + 2 * s + k] = 1.0
            r3[base + 32 + k, 256 + 96 + 2 * s + k] = 1.0
            for half in range(2):
                r3[base + 2 + 2 * k + half, 128 + 104 + k] = 0.125
                r3[base + 30 + 2 * k + half, 256 + 104 + k] = 0.125
    up = np.zeros((128, 128), np.float32)
    up0 = np.zeros((128, 128), np.float32)
    for out in range(128):
        step = -1 if out % 2 == 0 else 1
        centre = out // 2 + 1
        if 0 <= centre + step:
            up[centre, out] += 0.75
            up[centre + step, out] += 0.25
        centre = out // 2 + 2
        up0[centre, out] += 0.75
        up0[centre + step, out] += 0.25
    return tuple(m.astype(BF16) for m in (r1, r2, r3, up, up0))


def dot(a, b):
    return jnp.dot(a, b, preferred_element_type=F32)


def call(kernel, outs, args, scratch=(), scalars=1):
    specs = [pl.BlockSpec(memory_space=pltpu.SMEM)] * scalars
    specs += [pl.BlockSpec(memory_space=pltpu.VMEM)] * (len(args) - scalars)
    return pl.pallas_call(
        kernel,
        out_shape=[jax.ShapeDtypeStruct(shape, BF16) for shape in outs],
        in_specs=specs,
        out_specs=[pl.BlockSpec(memory_space=pltpu.VMEM)] * len(outs),
        scratch_shapes=list(scratch),
        compiler_params=pltpu.CompilerParams(vmem_limit_bytes=48 * 1024 * 1024),
        interpret=INTERPRET,
    )(*args)


def restrict_kernel(field, r1, r2, r3, x_out, t1_out, t2_out, t3_out, msg_out, rows):
    rows[...] = field[...].astype(F32).reshape(2048, LANES)
    for x in range(8):
        for y in range(8):
            x_out[x, y] = rows[pl.ds(x * 8 + y, 32, stride=64), :].astype(BF16)

    def four(ref, x, y):
        return jnp.concatenate(
            [ref[2 * x, 2 * y], ref[2 * x, 2 * y + 1], ref[2 * x + 1, 2 * y], ref[2 * x + 1, 2 * y + 1]],
            axis=1,
        )

    for x in range(4):
        left = jnp.concatenate([four(x_out, x, y) for y in range(4)], axis=0)
        t1_out[x] = dot(left, r1[...]).astype(BF16).reshape(4, 32, LANES)
    left = jnp.concatenate([four(t1_out, x, y) for x in range(2) for y in range(2)], axis=0)
    t2_out[...] = dot(left, r2[...]).astype(BF16).reshape(2, 2, 32, LANES)
    t3 = dot(four(t2_out, 0, 0), r3[...]).astype(BF16)
    t3_out[...] = t3[:, :128]
    msg_out[0] = t3[:, 128:256]
    msg_out[1] = t3[:, 256:]


def lanes():
    return lax.broadcasted_iota(jnp.int32, (32, LANES), 1)


def rolled(value, shift):
    shift %= LANES
    return pltpu.roll(value, shift, 1) if shift else value


def depth_kernel(flags, x_ref, t1, t2, t3, from_lo, from_hi, t1_out, t2_out, t3_out, lo_out, hi_out):
    lane = lanes()
    low = jnp.where(flags[4] > 0, from_lo[...].astype(F32), 0.0)
    high = jnp.where(flags[5] > 0, from_hi[...].astype(F32), 0.0)

    def joined(own, mask_lo, shift_lo, mask_hi, shift_hi):
        value = own.astype(F32)
        value = jnp.where(mask_lo, rolled(low, shift_lo), value)
        return jnp.where(mask_hi, rolled(high, shift_hi), value).astype(BF16)

    mask_lo = (lane >= 124) | (lane < 2)
    mask_hi = (lane >= 66) & (lane < 72)
    for x in range(4):
        for y in range(4):
            tile = 4 * x + y
            value = joined(t1[x, y], mask_lo, 124 - 6 * tile, mask_hi, 66 - 6 * tile)
            t1_out[x, y] = value
            (lo_out if x < 2 else hi_out)[8 + 4 * (x % 2) + y] = value
    for x in range(2):
        for y in range(2):
            tile = 2 * x + y
            value = joined(
                t2[x, y], lane < 2, 32 - 2 * tile, (lane >= 34) & (lane < 36), 34 - 96 - 2 * tile
            )
            t2_out[x, y] = value
            lo_out[16 + tile] = value
            hi_out[16 + tile] = value
    value = joined(t3[...], lane < 2, 24, (lane >= 18) & (lane < 20), 18 - 104)
    t3_out[...] = value
    lo_out[20] = value
    hi_out[20] = value
    lo_out[0:8] = x_ref[0]
    hi_out[0:8] = x_ref[7]


def kept(flag, value):
    return jnp.where(flag > 0, value, jnp.zeros_like(value))


def width_kernel(flags, x_ref, t1, t2, t3, xr_lo, xr_hi, xr_lo2, xr_hi2, lo_out, hi_out, two_out):
    has_lo, has_hi, has_lo2, has_hi2 = flags[0], flags[1], flags[6], flags[7]
    for out, fine_y, half_y in ((lo_out, 0, 0), (hi_out, 7, 2)):
        out[0] = kept(has_lo, xr_lo[fine_y])
        out[9] = kept(has_hi, xr_hi[fine_y])
        for x in range(8):
            out[1 + x] = x_ref[x, fine_y]
        for x in range(2):
            for y in range(2):
                out[10 + 2 * x + y] = kept(has_lo, xr_lo[8 + 4 * x + half_y + y])
                out[10 + 2 * (x + 6) + y] = kept(has_hi, xr_hi[8 + 4 * x + half_y + y])
                out[26 + 2 * x + y] = kept(has_lo, xr_lo[16 + 2 * x + y])
                out[26 + 2 * (x + 4) + y] = kept(has_hi, xr_hi[16 + 2 * x + y])
                out[26 + 2 * (x + 2) + y] = t2[x, y]
        for x in range(4):
            for y in range(2):
                out[10 + 2 * (x + 2) + y] = t1[x, half_y + y]
        row = (
            kept(has_lo2, xr_lo2[...]),
            kept(has_lo, xr_lo[20]),
            t3[...],
            kept(has_hi, xr_hi[20]),
            kept(has_hi2, xr_hi2[...]),
        )
        for x in range(5):
            out[38 + x] = row[x]
            two_out[x] = row[x]


def final_kernel(
    flags, x_ref, t1, t2, t3, xr_lo, xr_hi, xr_lo2, xr_hi2, yr_lo, yr_hi, yr_two,
    w0, mix, w1, w2, w3, up, up0, out_ref, f0, e0, f1, e1, e2, e3, v3, v2, v1, q1, rows,
):
    x_lo, x_hi, y_lo, y_hi, z_lo, z_hi, x_lo2, x_hi2, y_lo2, y_hi2 = (flags[i] for i in range(10))
    lane = lanes()

    def spread(ref, i, j, value):
        wide = value.astype(F32)
        ref[i, j, 0:32] = rolled(wide, 1).astype(BF16)
        ref[i, j, 32:64] = value
        ref[i, j, 64:96] = rolled(wide, -1).astype(BF16)

    for i in range(5):
        spread(e3, i, 0, kept(y_lo2, yr_two[i]))
        spread(e3, i, 1, kept(y_lo, yr_lo[38 + i]))
        spread(e3, i, 3, kept(y_hi, yr_hi[38 + i]))
        spread(e3, i, 4, kept(y_hi2, yr_two[i]))
    spread(e3, 0, 2, kept(x_lo2, xr_lo2[...]))
    spread(e3, 1, 2, kept(x_lo, xr_lo[20]))
    spread(e3, 2, 2, t3[...])
    spread(e3, 3, 2, kept(x_hi, xr_hi[20]))
    spread(e3, 4, 2, kept(x_hi2, xr_hi2[...]))
    for i in range(6):
        for k in range(2):
            spread(e2, i, k, kept(y_lo, yr_lo[26 + 2 * i + k]))
            spread(e2, i, 4 + k, kept(y_hi, yr_hi[26 + 2 * i + k]))
    for i in range(2):
        for k in range(2):
            spread(e2, i, 2 + k, kept(x_lo, xr_lo[16 + 2 * i + k]))
            spread(e2, 2 + i, 2 + k, t2[i, k])
            spread(e2, 4 + i, 2 + k, kept(x_hi, xr_hi[16 + 2 * i + k]))
    for i in range(8):
        for k in range(2):
            f1[i, k] = kept(y_lo, yr_lo[10 + 2 * i + k])
            f1[i, 6 + k] = kept(y_hi, yr_hi[10 + 2 * i + k])
    for i in range(2):
        for k in range(4):
            f1[i, 2 + k] = kept(x_lo, xr_lo[8 + 4 * i + k])
            f1[6 + i, 2 + k] = kept(x_hi, xr_hi[8 + 4 * i + k])
    f1[2:6, 2:6] = t1[...]

    def fill1(i, carry):
        for j in range(8):
            spread(e1, i, j, f1[i, j])
        return carry

    lax.fori_loop(0, 8, fill1, 0)

    for i in range(10):
        f0[i, 0] = kept(y_lo, yr_lo[i])
        f0[i, 9] = kept(y_hi, yr_hi[i])
    for k in range(8):
        f0[0, 1 + k] = kept(x_lo, xr_lo[k])
        f0[9, 1 + k] = kept(x_hi, xr_hi[k])
    f0[1:9, 1:9] = x_ref[...]

    def fill0(half, carry):
        for part in range(2):
            i = 2 * half + part
            coarse = half + 1 + part
            sx = 1 - part
            for j in range(10):
                s = 2 * sx + (j + 1) % 2
                value = f0[i, j]
                wide = value.astype(F32)
                column = f1[coarse, (j + 1) // 2 + 1].astype(F32)
                e0[i, j, 0:32] = jnp.where(lane == 0, rolled(column, 4 - s), rolled(wide, 1)).astype(BF16)
                e0[i, j, 32:64] = value
                e0[i, j, 64:96] = jnp.where(lane == 127, rolled(column, 59 - s), rolled(wide, -1)).astype(BF16)
        return carry

    lax.fori_loop(0, 5, fill0, 0)

    def gathered(ref, x, ys):
        return jnp.concatenate(
            [
                jnp.concatenate([ref[x + d, y : y + 3].reshape(288, LANES) for y in ys], axis=1)
                for d in range(3)
            ],
            axis=0,
        )

    def weighted(weight, value):
        return lax.dot_general(weight, value, (((0,), (0,)), ((), ())), preferred_element_type=F32)

    def along(before, centre, after):
        return [0.75 * centre + 0.25 * before, 0.75 * centre + 0.25 * after]

    def limits(count):
        inside = (lane >= 1) & (lane <= count + 2)
        inside &= (lane != 1) | (z_lo > 0)
        return inside & ((lane != count + 2) | (z_hi > 0))

    def cell_flag(position, last, lo, hi):
        return lo if position == 0 else hi if position == last else None

    def prolonged(ref, count):
        wide = dot(ref[...].reshape(count * count * 32, LANES), up[...]).reshape(count, count, 32, LANES)
        made = 2 * count - 2

        def refined(cells):
            out = []
            for k in range(made):
                cell = k - 1
                centre = cell // 2 + 1
                other = centre - 1 if cell % 2 == 0 else centre + 1
                out.append(0.75 * cells[centre] + 0.25 * cells[other])
            return out

        by_x = refined([wide[i] for i in range(count)])
        return [refined([row[j] for j in range(count)]) for row in by_x]

    def level(e_ref, w_ref, v_ref, size, cells, above):
        keep = limits(cells)
        for i in range(size):
            for j in range(0, size, 2):
                ys = [j, j + 1] if j + 1 < size else [j]
                value = weighted(w_ref[...], gathered(e_ref, i, ys))
                for n, y in enumerate(ys):
                    part = value[:, LANES * n : LANES * (n + 1)]
                    if above is not None:
                        part = part + above[i][y]
                    good = keep
                    for flag in (cell_flag(i, size - 1, x_lo, x_hi), cell_flag(y, size - 1, y_lo, y_hi)):
                        if flag is not None:
                            good = good & (flag > 0)
                    v_ref[i, y] = jnp.where(good, part, 0.0).astype(BF16)

    level(e3, w3, v3, 3, 16, None)
    level(e2, w2, v2, 4, 32, prolonged(v3, 3))
    level(e1, w1, v1, 6, 64, prolonged(v2, 4))
    for i in range(6):
        q1[i] = dot(v1[i].reshape(6 * 32, LANES), up0[...]).reshape(6, 32, LANES)

    weight = jnp.concatenate([w0[...], mix[...]], axis=0)

    def fine(c, carry):
        for part in range(2):
            x = 2 * c + part
            row = 0.75 * q1[c + 1] + 0.25 * q1[c + 2 * part]
            for y in range(0, 8, 2):
                middle = jnp.concatenate([f0[x + 1, y + 1], f0[x + 1, y + 2]], axis=1)
                value = weighted(weight, jnp.concatenate([gathered(e0, x, [y, y + 1]), middle], axis=0))
                centre = y // 2 + 1
                for n, extra in enumerate(along(row[centre - 1], row[centre], row[centre + 1])):
                    total = value[:, LANES * n : LANES * (n + 1)] + extra
                    rows[pl.ds(x * 8 + y + n, 32, stride=64), :] = jax.nn.gelu(total, approximate=True)
        return carry

    lax.fori_loop(0, 4, fine, 0)
    out_ref[...] = rows[...].reshape(32, 8, 8, LANES).astype(BF16)


def turned(value, axis, step):
    count = lax.axis_size(axis)
    return lax.ppermute(value, axis, [(i, (i + step) % count) for i in range(count)])


def on_device(field, mixing, kernel_fine, kernel_half, kernel_quarter, kernel_eighth):
    gx, gy, gz = (lax.axis_index(a) for a in ("gx", "gy", "gz"))
    nx, ny, nz = (lax.axis_size(a) for a in ("gx", "gy", "gz"))
    slot = lax.iota(jnp.int32, 16)
    place = jnp.where((slot < 2) | (slot == 6) | (slot == 7), gx, jnp.where((slot == 4) | (slot == 5), gz, gy))
    first = np.array([1, 0, 1, 0, 1, 0, 2, 0, 2, 0] + [0] * 6, np.int32)
    last = np.array([nx, nx - 1, ny, ny - 1, nz, nz - 1, nx, nx - 2, ny, ny - 2] + [99] * 6, np.int32)
    flags = ((place >= first) & (place < last)).astype(jnp.int32)
    r1, r2, r3, up, up0 = (jnp.asarray(m) for m in tables())
    tile = (32, LANES)

    x_own, t1, t2, t3, msg = call(
        restrict_kernel,
        [(8, 8) + tile, (4, 4) + tile, (2, 2) + tile, tile, (2,) + tile],
        [field, r1, r2, r3],
        [pltpu.VMEM((2048, LANES), F32)],
        0,
    )
    from_hi = turned(msg[0], "gz", -1)
    from_lo = turned(msg[1], "gz", 1)
    t1, t2, t3, x_msg_lo, x_msg_hi = call(
        depth_kernel,
        [(4, 4) + tile, (2, 2) + tile, tile, (21,) + tile, (21,) + tile],
        [flags, x_own, t1, t2, t3, from_lo, from_hi],
    )
    xr_hi = turned(x_msg_lo, "gx", -1)
    xr_lo = turned(x_msg_hi, "gx", 1)
    xr_hi2 = turned(t3, "gx", -2)
    xr_lo2 = turned(t3, "gx", 2)
    y_msg_lo, y_msg_hi, two = call(
        width_kernel,
        [(43,) + tile, (43,) + tile, (5,) + tile],
        [flags, x_own, t1, t2, t3, xr_lo, xr_hi, xr_lo2, xr_hi2],
    )
    yr_hi = turned(y_msg_lo, "gy", -1)
    yr_lo = turned(y_msg_hi, "gy", 1)
    assert ny == 4
    yr_two = turned(two, "gy", 2)
    flat = [k.reshape(864, 32) for k in (kernel_fine, kernel_half, kernel_quarter, kernel_eighth)]
    (out,) = call(
        final_kernel,
        [(32, 8, 8, LANES)],
        [flags, x_own, t1, t2, t3, xr_lo, xr_hi, xr_lo2, xr_hi2, yr_lo, yr_hi, yr_two,
         flat[0], mixing.T, flat[1], flat[2], flat[3], up, up0],
        [
            pltpu.VMEM((10, 10) + tile, BF16),
            pltpu.VMEM((10, 10, 96, LANES), BF16),
            pltpu.VMEM((8, 8) + tile, BF16),
            pltpu.VMEM((8, 8, 96, LANES), BF16),
            pltpu.VMEM((6, 6, 96, LANES), BF16),
            pltpu.VMEM((5, 5, 96, LANES), BF16),
            pltpu.VMEM((3, 3) + tile, BF16),
            pltpu.VMEM((4, 4) + tile, BF16),
            pltpu.VMEM((6, 6) + tile, BF16),
            pltpu.VMEM((6, 6) + tile, F32),
            pltpu.VMEM((2048, LANES), F32),
        ],
    )
    return out


def solution(mesh):
    placed = (P(None, "gx", "gy", "gz"), P(), P(), P(), P(), P())
    return jax.shard_map(
        on_device, mesh=mesh, in_specs=placed, out_specs=P(None, "gx", "gy", "gz"), check_vma=False
    )
```

```python
import jax
import jax.numpy as jnp
import numpy as np
from jax import lax
from jax.experimental import pallas as pl
from jax.experimental.pallas import tpu as pltpu
from jax.sharding import PartitionSpec as P

INTERPRET = False
F32, BF16 = jnp.float32, jnp.bfloat16
LANES = 128


def tables():
    r1 = np.zeros((512, 128), np.float32)
    r2 = np.zeros((512, 128), np.float32)
    r3 = np.zeros((512, 384), np.float32)
    for s in range(4):
        base = s * 128
        for z in range(128):
            r1[base + z, 2 + z // 2] = 0.125
        r1[base, 72 + s] = 1.0
        r1[base + 127, 76 + s] = 1.0
        for z in range(64):
            r2[base + 2 + z, 2 + z // 2] = 0.125
        for k, lane in enumerate((2, 3, 72, 73, 74, 75)):
            r2[base + lane, 40 + 6 * s + k] = 1.0
        for k, lane in enumerate((76, 77, 78, 79, 64, 65)):
            r2[base + lane, 64 + 6 * s + k] = 1.0
        for z in range(32):
            r3[base + 2 + z, 2 + z // 2] = 0.125
        for sub in range(4):
            tile = (2 * (s // 2) + sub // 2) * 4 + 2 * (s % 2) + sub % 2
            for k in range(6):
                r3[base + 40 + 6 * sub + k, 128 + 6 * tile + k] = 1.0
                r3[base + 64 + 6 * sub + k, 256 + 6 * tile + k] = 1.0
        for k in range(2):
            r3[base + 2 + k, 128 + 96 + 2 * s + k] = 1.0
            r3[base + 32 + k, 256 + 96 + 2 * s + k] = 1.0
            for half in range(2):
                r3[base + 2 + 2 * k + half, 128 + 104 + k] = 0.125
                r3[base + 30 + 2 * k + half, 256 + 104 + k] = 0.125
    up = np.zeros((128, 128), np.float32)
    up0 = np.zeros((128, 128), np.float32)
    for out in range(128):
        step = -1 if out % 2 == 0 else 1
        centre = out // 2 + 1
        if 0 <= centre + step:
            up[centre, out] += 0.75
            up[centre + step, out] += 0.25
        centre = out // 2 + 2
        up0[centre, out] += 0.75
        up0[centre + step, out] += 0.25
    return tuple(m.astype(BF16) for m in (np.concatenate([r1, r2, r3], axis=1), up, up0))


def dot(a, b):
    return jnp.dot(a, b, preferred_element_type=F32)


def call(kernel, outs, args, scratch=(), scalars=1, space=pltpu.VMEM, kind=BF16, flops=1 << 20):
    specs = [pl.BlockSpec(memory_space=pltpu.SMEM)] * scalars
    specs += [pl.BlockSpec(memory_space=space)] * (len(args) - scalars)
    return pl.pallas_call(
        kernel,
        out_shape=[jax.ShapeDtypeStruct(shape, kind) for shape in outs],
        in_specs=specs,
        out_specs=[pl.BlockSpec(memory_space=pltpu.VMEM)] * len(outs),
        scratch_shapes=list(scratch),
        compiler_params=pltpu.CompilerParams(vmem_limit_bytes=48 * 1024 * 1024),
        cost_estimate=pl.CostEstimate(flops=flops, transcendentals=0, bytes_accessed=1 << 20),
        interpret=INTERPRET,
    )(*args)


def restrict_kernel(field_hbm, table_hbm, x_out, t1_out, t2_out, t3_out, msg_out, field, table, rows, sems):
    copies = [
        pltpu.make_async_copy(field_hbm, field, sems.at[0]),
        pltpu.make_async_copy(table_hbm, table, sems.at[1]),
    ]
    for copy in copies:
        copy.start()
    copies[0].wait()
    rows[...] = field[...].astype(F32).reshape(2048, LANES)
    for x in range(8):
        for y in range(8):
            x_out[x, y] = rows[pl.ds(x * 8 + y, 32, stride=64), :].astype(BF16)
    copies[1].wait()

    def four(ref, x, y):
        return jnp.concatenate(
            [ref[2 * x, 2 * y], ref[2 * x, 2 * y + 1], ref[2 * x + 1, 2 * y], ref[2 * x + 1, 2 * y + 1]],
            axis=1,
        )

    for x in range(4):
        left = jnp.concatenate([four(x_out, x, y) for y in range(4)], axis=0)
        t1_out[x] = dot(left, table[:, 0:128]).astype(BF16).reshape(4, 32, LANES)
    left = jnp.concatenate([four(t1_out, x, y) for x in range(2) for y in range(2)], axis=0)
    t2_out[...] = dot(left, table[:, 128:256]).astype(BF16).reshape(2, 2, 32, LANES)
    t3 = dot(four(t2_out, 0, 0), table[:, 256:640]).astype(BF16)
    t3_out[...] = t3[:, :128]
    msg_out[0] = t3[:, 128:256]
    msg_out[1] = t3[:, 256:]


def lanes():
    return lax.broadcasted_iota(jnp.int32, (32, LANES), 1)


def rolled(value, shift):
    shift %= LANES
    return pltpu.roll(value, shift, 1) if shift else value


def depth_kernel(flags, x_ref, t1, t2, t3, from_lo, from_hi, t1_out, t2_out, t3_out, lo_out, hi_out):
    lane = lanes()
    low = jnp.where(flags[4] > 0, from_lo[...].astype(F32), 0.0)
    high = jnp.where(flags[5] > 0, from_hi[...].astype(F32), 0.0)

    def joined(own, mask_lo, shift_lo, mask_hi, shift_hi):
        value = own.astype(F32)
        value = jnp.where(mask_lo, rolled(low, shift_lo), value)
        return jnp.where(mask_hi, rolled(high, shift_hi), value)

    extra = []
    for x in range(2):
        for y in range(2):
            tile = 2 * x + y
            value = joined(
                t2[x, y], lane < 2, 32 - 2 * tile, (lane >= 34) & (lane < 36), 34 - 96 - 2 * tile
            )
            t2_out[x, y] = value.astype(BF16)
            extra.append(rolled(value, 72))
    value = joined(t3[...], lane < 2, 24, (lane >= 18) & (lane < 20), 18 - 104)
    t3_out[...] = value.astype(BF16)
    extra.append(rolled(value, 72))
    free = (lane >= 72) & (lane < 108)
    mask_lo = (lane >= 124) | (lane < 2)
    mask_hi = (lane >= 66) & (lane < 72)
    for x in range(4):
        for y in range(4):
            tile = 4 * x + y
            value = joined(t1[x, y], mask_lo, 124 - 6 * tile, mask_hi, 66 - 6 * tile)
            t1_out[x, y] = value.astype(BF16)
            k = tile % 8
            if k < 5:
                value = jnp.where(free, extra[k], value)
            (lo_out if x < 2 else hi_out)[8 + k] = value.astype(BF16)
    lo_out[0:8] = x_ref[0]
    hi_out[0:8] = x_ref[7]


def kept(flag, value):
    return jnp.where(flag > 0, value, jnp.zeros_like(value))


def width_kernel(flags, x_ref, t1, t2, t3, xr_lo, xr_hi, xr_lo2, xr_hi2, lo_out, hi_out, two_out):
    has_lo, has_hi, has_lo2, has_hi2 = flags[0], flags[1], flags[6], flags[7]
    lane = lanes()
    free = (lane >= 72) & (lane < 124)
    row = [
        rolled(kept(has_lo2, xr_lo2[...]).astype(F32), 0),
        rolled(kept(has_lo, xr_lo[12]).astype(F32), -72),
        t3[...].astype(F32),
        rolled(kept(has_hi, xr_hi[12]).astype(F32), -72),
        rolled(kept(has_hi2, xr_hi2[...]).astype(F32), 0),
    ]
    two = row[0]
    for i in range(1, 5):
        two = jnp.where(lane < 20 * i, two, rolled(row[i], 20 * i))
    two_out[...] = two.astype(BF16)
    coarse = [rolled(two, 72), rolled(two, 72 - 40), rolled(two, 72 - 80)]

    for out, fine_y, half_y in ((lo_out, 0, 0), (hi_out, 7, 2)):
        out[0] = kept(has_lo, xr_lo[fine_y])
        out[9] = kept(has_hi, xr_hi[fine_y])
        for x in range(8):
            out[1 + x] = x_ref[x, fine_y]
        for i in range(8):
            for k in range(2):
                y = half_y + k
                if i < 2:
                    value = kept(has_lo, xr_lo[8 + 4 * i + y])
                elif i < 6:
                    value = t1[i - 2, y]
                else:
                    value = kept(has_hi, xr_hi[8 + 4 * (i - 6) + y])
                if i < 2:
                    extra = kept(has_lo, xr_lo[8 + 2 * i + k]).astype(F32)
                elif i < 4:
                    extra = rolled(t2[i - 2, k].astype(F32), 72)
                elif i < 6:
                    extra = kept(has_hi, xr_hi[8 + 2 * (i - 4) + k]).astype(F32)
                else:
                    spot = 2 * (i - 6) + k
                    extra = coarse[spot] if spot < 3 else None
                if extra is not None:
                    value = jnp.where(free, extra, value.astype(F32)).astype(BF16)
                out[10 + 2 * i + k] = value


def taps(ref, x, ys):
    return jnp.concatenate(
        [
            jnp.concatenate([ref[x + d, y : y + 3].reshape(288, LANES) for y in ys], axis=1)
            for d in range(3)
        ],
        axis=0,
    )


def weighted(weight, value):
    return lax.dot_general(weight, value, (((0,), (0,)), ((), ())), preferred_element_type=F32)


def spread(ref, i, j, value, base=0, lo=None, hi=None):
    lane = lanes()
    wide = value.astype(F32)
    before, after = rolled(wide, base + 1), rolled(wide, base - 1)
    if lo is not None:
        before = jnp.where(lane == 0, lo, before)
        after = jnp.where(lane == LANES - 1, hi, after)
    ref[i, j, 0:32] = before.astype(BF16)
    ref[i, j, 32:64] = rolled(wide, base).astype(BF16) if base else value
    ref[i, j, 64:96] = after.astype(BF16)


def fine_kernel(flags, x_ref, t1, xr_lo, xr_hi, w0, mix, acc_out, e0):
    zero = jnp.zeros((96, LANES), BF16)
    for i in range(10):
        e0[i, 0] = zero
        e0[i, 9] = zero
    for k in range(8):
        s = k % 2
        column = kept(flags[0], xr_lo[8 + 4 + k // 2]).astype(F32)
        spread(e0, 0, 1 + k, kept(flags[0], xr_lo[k]), 0, rolled(column, 2 - s), rolled(column, 57 - s))
        column = kept(flags[1], xr_hi[8 + k // 2]).astype(F32)
        spread(e0, 9, 1 + k, kept(flags[1], xr_hi[k]), 0, rolled(column, 4 - s), rolled(column, 59 - s))

    def fill(c, carry):
        for part in range(2):
            for k in range(8):
                s = 2 * part + k % 2
                column = t1[c, k // 2].astype(F32)
                spread(
                    e0, 2 * c + part + 1, 1 + k, x_ref[2 * c + part, k], 0,
                    rolled(column, 4 - s), rolled(column, 59 - s),
                )
        return carry

    lax.fori_loop(0, 4, fill, 0)
    weight = jnp.concatenate([w0[...], mix[...]], axis=0)

    def fine(x, carry):
        for y in range(0, 8, 2):
            middle = jnp.concatenate([x_ref[x, y], x_ref[x, y + 1]], axis=1)
            value = weighted(weight, jnp.concatenate([taps(e0, x, [y, y + 1]), middle], axis=0))
            acc_out[x, y] = value[:, :LANES]
            acc_out[x, y + 1] = value[:, LANES:]
        return carry

    lax.fori_loop(0, 8, fine, 0)


def final_kernel(
    flags, acc, t1, t2, t3, xr_lo, xr_hi, xr_lo2, xr_hi2, yr_lo, yr_hi, yr_two,
    w0, w1, w2, w3, up, up0, out_ref, ey, edge, e1, e2, e3, v3, v2, v1, q1, rows,
):
    x_lo, x_hi, y_lo, y_hi, z_lo, z_hi, x_lo2, x_hi2, y_lo2, y_hi2 = (flags[i] for i in range(10))
    lane = lanes()

    for i in range(5):
        spread(e3, i, 0, kept(y_lo2, yr_two[...]), -20 * i)
        spread(e3, i, 1, kept(y_lo, yr_lo[22 + i // 2]), -72 - 20 * (i % 2))
        spread(e3, i, 3, kept(y_hi, yr_hi[22 + i // 2]), -72 - 20 * (i % 2))
        spread(e3, i, 4, kept(y_hi2, yr_two[...]), -20 * i)
    spread(e3, 0, 2, kept(x_lo2, xr_lo2[...]))
    spread(e3, 1, 2, kept(x_lo, xr_lo[12]), -72)
    spread(e3, 2, 2, t3[...])
    spread(e3, 3, 2, kept(x_hi, xr_hi[12]), -72)
    spread(e3, 4, 2, kept(x_hi2, xr_hi2[...]))
    for i in range(6):
        for k in range(2):
            spread(e2, i, k, kept(y_lo, yr_lo[10 + 2 * i + k]), -72)
            spread(e2, i, 4 + k, kept(y_hi, yr_hi[10 + 2 * i + k]), -72)
    for i in range(2):
        for k in range(2):
            spread(e2, i, 2 + k, kept(x_lo, xr_lo[8 + 2 * i + k]), -72)
            spread(e2, 2 + i, 2 + k, t2[i, k])
            spread(e2, 4 + i, 2 + k, kept(x_hi, xr_hi[8 + 2 * i + k]), -72)
    for i in range(8):
        for k in range(2):
            spread(e1, i, k, kept(y_lo, yr_lo[10 + 2 * i + k]))
            spread(e1, i, 6 + k, kept(y_hi, yr_hi[10 + 2 * i + k]))
    for k in range(4):
        for i in range(2):
            spread(e1, i, 2 + k, kept(x_lo, xr_lo[8 + 4 * i + k]))
            spread(e1, 6 + i, 2 + k, kept(x_hi, xr_hi[8 + 4 * i + k]))
        for i in range(4):
            spread(e1, 2 + i, 2 + k, t1[i, k])
    for i in range(10):
        sx = (i + 1) % 2
        coarse = (i + 1) // 2 + 1
        for side, ref, flag, row, s in ((0, yr_lo, y_lo, 1, 2 * sx + 1), (1, yr_hi, y_hi, 0, 2 * sx)):
            column = kept(flag, ref[10 + 2 * coarse + row]).astype(F32)
            spread(ey, side, i, kept(flag, ref[i]), 0, rolled(column, 4 - s), rolled(column, 59 - s))
    for side, dy in ((0, 0), (1, 2)):
        weight = jnp.concatenate([w0[96 * (3 * dx + dy) : 96 * (3 * dx + dy) + 96] for dx in range(3)], axis=0)
        for x in range(0, 8, 2):
            value = jnp.concatenate(
                [ey[side, x : x + 3].reshape(288, LANES), ey[side, x + 1 : x + 4].reshape(288, LANES)], axis=1
            )
            value = weighted(weight, value)
            edge[side, x] = value[:, :LANES]
            edge[side, x + 1] = value[:, LANES:]

    def along(before, centre, after):
        return [0.75 * centre + 0.25 * before, 0.75 * centre + 0.25 * after]

    def limits(count):
        inside = (lane >= 1) & (lane <= count + 2)
        inside &= (lane != 1) | (z_lo > 0)
        return inside & ((lane != count + 2) | (z_hi > 0))

    def cell_flag(position, last, lo, hi):
        return lo if position == 0 else hi if position == last else None

    def prolonged(ref, count):
        wide = dot(ref[...].reshape(count * count * 32, LANES), up[...]).reshape(count, count, 32, LANES)

        def refined(cells):
            out = []
            for k in range(2 * count - 2):
                cell = k - 1
                centre = cell // 2 + 1
                other = centre - 1 if cell % 2 == 0 else centre + 1
                out.append(0.75 * cells[centre] + 0.25 * cells[other])
            return out

        by_x = refined([wide[i] for i in range(count)])
        return [refined([row[j] for j in range(count)]) for row in by_x]

    def level(e_ref, w_ref, v_ref, size, cells, above):
        keep = limits(cells)
        for i in range(size):
            for j in range(0, size, 2):
                ys = [j, j + 1] if j + 1 < size else [j]
                value = weighted(w_ref[...], taps(e_ref, i, ys))
                for n, y in enumerate(ys):
                    part = value[:, LANES * n : LANES * (n + 1)]
                    if above is not None:
                        part = part + above[i][y]
                    good = keep
                    for flag in (cell_flag(i, size - 1, x_lo, x_hi), cell_flag(y, size - 1, y_lo, y_hi)):
                        if flag is not None:
                            good = good & (flag > 0)
                    v_ref[i, y] = jnp.where(good, part, 0.0).astype(BF16)

    level(e3, w3, v3, 3, 16, None)
    level(e2, w2, v2, 4, 32, prolonged(v3, 3))
    level(e1, w1, v1, 6, 64, prolonged(v2, 4))
    for i in range(6):
        q1[i] = dot(v1[i].reshape(6 * 32, LANES), up0[...]).reshape(6, 32, LANES)

    def fine(c, carry):
        for part in range(2):
            x = 2 * c + part
            row = 0.75 * q1[c + 1] + 0.25 * q1[c + 2 * part]
            for y in range(0, 8, 2):
                centre = y // 2 + 1
                for n, extra in enumerate(along(row[centre - 1], row[centre], row[centre + 1])):
                    total = acc[x, y + n] + extra
                    if y + n == 0:
                        total = total + edge[0, x]
                    if y + n == 7:
                        total = total + edge[1, x]
                    rows[pl.ds(x * 8 + y + n, 32, stride=64), :] = jax.nn.gelu(total, approximate=True)
        return carry

    lax.fori_loop(0, 4, fine, 0)
    out_ref[...] = rows[...].reshape(32, 8, 8, LANES).astype(BF16)


def turned(value, axis, step):
    count = lax.axis_size(axis)
    return lax.ppermute(value, axis, [(i, (i + step) % count) for i in range(count)])


def on_device(field, mixing, kernel_fine, kernel_half, kernel_quarter, kernel_eighth):
    gx, gy, gz = (lax.axis_index(a) for a in ("gx", "gy", "gz"))
    nx, ny, nz = (lax.axis_size(a) for a in ("gx", "gy", "gz"))
    slot = lax.iota(jnp.int32, 16)
    place = jnp.where((slot < 2) | (slot == 6) | (slot == 7), gx, jnp.where((slot == 4) | (slot == 5), gz, gy))
    first = np.array([1, 0, 1, 0, 1, 0, 2, 0, 2, 0] + [0] * 6, np.int32)
    last = np.array([nx, nx - 1, ny, ny - 1, nz, nz - 1, nx, nx - 2, ny, ny - 2] + [99] * 6, np.int32)
    flags = ((place >= first) & (place < last)).astype(jnp.int32)
    table, up, up0 = (jnp.asarray(m) for m in tables())
    tile = (32, LANES)

    x_own, t1, t2, t3, msg = call(
        restrict_kernel,
        [(8, 8) + tile, (4, 4) + tile, (2, 2) + tile, tile, (2,) + tile],
        [field, table],
        [
            pltpu.VMEM((32, 8, 8, LANES), BF16),
            pltpu.VMEM((512, 640), BF16),
            pltpu.VMEM((2048, LANES), F32),
            pltpu.SemaphoreType.DMA((2,)),
        ],
        0,
        pltpu.HBM,
    )
    from_hi = turned(msg[0], "gz", -1)
    from_lo = turned(msg[1], "gz", 1)
    t1, t2, t3, x_msg_lo, x_msg_hi = call(
        depth_kernel,
        [(4, 4) + tile, (2, 2) + tile, tile, (16,) + tile, (16,) + tile],
        [flags, x_own, t1, t2, t3, from_lo, from_hi],
    )
    xr_hi = turned(x_msg_lo, "gx", -1)
    xr_lo = turned(x_msg_hi, "gx", 1)
    xr_hi2 = turned(t3, "gx", -2)
    xr_lo2 = turned(t3, "gx", 2)
    y_msg_lo, y_msg_hi, two = call(
        width_kernel,
        [(26,) + tile, (26,) + tile, tile],
        [flags, x_own, t1, t2, t3, xr_lo, xr_hi, xr_lo2, xr_hi2],
    )
    yr_hi = turned(y_msg_lo, "gy", -1)
    yr_lo = turned(y_msg_hi, "gy", 1)
    assert ny == 4
    yr_two = turned(two, "gy", 2)
    flat = [k.reshape(864, 32) for k in (kernel_fine, kernel_half, kernel_quarter, kernel_eighth)]
    (acc,) = call(
        fine_kernel,
        [(8, 8) + tile],
        [flags, x_own, t1, xr_lo, xr_hi, flat[0], mixing.T],
        [pltpu.VMEM((10, 10, 96, LANES), BF16)],
        kind=F32,
        flops=1 << 30,
    )
    (out,) = call(
        final_kernel,
        [(32, 8, 8, LANES)],
        [flags, acc, t1, t2, t3, xr_lo, xr_hi, xr_lo2, xr_hi2, yr_lo, yr_hi, yr_two,
         *flat, up, up0],
        [
            pltpu.VMEM((2, 10, 96, LANES), BF16),
            pltpu.VMEM((2, 8) + tile, F32),
            pltpu.VMEM((8, 8, 96, LANES), BF16),
            pltpu.VMEM((6, 6, 96, LANES), BF16),
            pltpu.VMEM((5, 5, 96, LANES), BF16),
            pltpu.VMEM((3, 3) + tile, BF16),
            pltpu.VMEM((4, 4) + tile, BF16),
            pltpu.VMEM((6, 6) + tile, BF16),
            pltpu.VMEM((6, 6) + tile, F32),
            pltpu.VMEM((2048, LANES), F32),
        ],
    )
    return out


def solution(mesh):
    placed = (P(None, "gx", "gy", "gz"), P(), P(), P(), P(), P())
    return jax.shard_map(
        on_device, mesh=mesh, in_specs=placed, out_specs=P(None, "gx", "gy", "gz"), check_vma=False
    )
```

```python
import jax
import jax.numpy as jnp
import numpy as np
from jax import lax
from jax.experimental import pallas as pl
from jax.experimental.pallas import tpu as pltpu
from jax.sharding import PartitionSpec as P

INTERPRET = False
F32, BF16 = jnp.float32, jnp.bfloat16
LANES = 128


def tables():
    up = np.zeros((128, 128), np.float32)
    up0 = np.zeros((128, 128), np.float32)
    for out in range(128):
        step = -1 if out % 2 == 0 else 1
        centre = out // 2 + 1
        if 0 <= centre + step:
            up[centre, out] += 0.75
            up[centre + step, out] += 0.25
        centre = out // 2 + 2
        up0[centre, out] += 0.75
        up0[centre + step, out] += 0.25
    return tuple(m.astype(BF16) for m in (up, up0))


def restrictions(table):
    row = lax.broadcasted_iota(jnp.int32, (512, LANES), 0)
    lane = lax.broadcasted_iota(jnp.int32, (1, LANES), 1)
    spot = row & 127
    base = row - spot
    eighth = jnp.float32(0.125)

    def put(k, *terms):
        value = jnp.zeros((512, LANES), F32)
        for mask, amount in terms:
            value = jnp.where(mask, amount, value)
        table[:, LANES * k : LANES * (k + 1)] = value.astype(BF16)

    def at(target, valid):
        return row == jnp.where(valid, target, -1)

    put(
        0,
        ((spot >> 1) + 2 == lane, eighth),
        (at((lane - 72) * 128, (lane >= 72) & (lane < 76)), 1.0),
        (at((lane - 76) * 128 + 127, (lane >= 76) & (lane < 80)), 1.0),
    )
    halves = ((spot - 2) >> 1) + 2 == lane
    sub = ((lane - 40) * 43) >> 8
    k = lane - 40 - 6 * sub
    low = at(sub * 128 + jnp.where(k < 2, 2 + k, 70 + k), (lane >= 40) & (lane < 64))
    sub = ((lane - 64) * 43) >> 8
    k = lane - 64 - 6 * sub
    high = at(sub * 128 + jnp.where(k < 4, 76 + k, 60 + k), (lane >= 64) & (lane < 88))
    put(1, (halves & (spot < 66) & (spot >= 2), eighth), (low, 1.0), (high, 1.0))
    put(2, (halves & (spot < 34) & (spot >= 2), eighth))
    tile = (lane * 43) >> 8
    k = lane - 6 * tile
    quad = (tile >> 3) * 2 + ((tile & 3) >> 1)
    sub = ((tile >> 2) & 1) * 2 + (tile & 1)
    last = (lane - 104) * 2
    for n, start, own, own3 in ((3, 40, 2, 2), (4, 64, 32, 30)):
        target = jnp.where(lane < 96, quad * 128 + start + 6 * sub + k, ((lane - 96) >> 1) * 128 + own + (lane & 1))
        tail = ((spot - own3) & ~1) == jnp.where((lane >= 104) & (lane < 106), last, -1000)
        put(n, (at(target, lane < 104), 1.0), (tail, eighth))


def dot(a, b):
    return jnp.dot(a, b, preferred_element_type=F32)


def call(kernel, outs, args, scratch=(), scalars=1, kind=BF16, flops=1 << 20):
    specs = [pl.BlockSpec(memory_space=pltpu.SMEM)] * scalars
    specs += [pl.BlockSpec(memory_space=pltpu.VMEM)] * (len(args) - scalars)
    return pl.pallas_call(
        kernel,
        out_shape=[jax.ShapeDtypeStruct(shape, kind) for shape in outs],
        in_specs=specs,
        out_specs=[pl.BlockSpec(memory_space=pltpu.VMEM)] * len(outs),
        scratch_shapes=list(scratch),
        compiler_params=pltpu.CompilerParams(vmem_limit_bytes=48 * 1024 * 1024),
        cost_estimate=pl.CostEstimate(flops=flops, transcendentals=0, bytes_accessed=1 << 20),
        interpret=INTERPRET,
    )(*args)


def restrict_kernel(field, table, x_out, t1_out, t2_out, t3_out, msg_out, rows):
    rows[...] = field[...].astype(F32).reshape(2048, LANES)
    for x in range(8):
        for y in range(8):
            x_out[x, y] = rows[pl.ds(x * 8 + y, 32, stride=64), :].astype(BF16)

    def four(ref, x, y):
        return jnp.concatenate(
            [ref[2 * x, 2 * y], ref[2 * x, 2 * y + 1], ref[2 * x + 1, 2 * y], ref[2 * x + 1, 2 * y + 1]],
            axis=1,
        )

    for x in range(4):
        left = jnp.concatenate([four(x_out, x, y) for y in range(4)], axis=0)
        t1_out[x] = dot(left, table[:, 0:128]).astype(BF16).reshape(4, 32, LANES)
    left = jnp.concatenate([four(t1_out, x, y) for x in range(2) for y in range(2)], axis=0)
    t2_out[...] = dot(left, table[:, 128:256]).astype(BF16).reshape(2, 2, 32, LANES)
    t3 = dot(four(t2_out, 0, 0), table[:, 256:640]).astype(BF16)
    t3_out[...] = t3[:, :128]
    msg_out[0] = t3[:, 128:256]
    msg_out[1] = t3[:, 256:]


def lanes():
    return lax.broadcasted_iota(jnp.int32, (32, LANES), 1)


def rolled(value, shift):
    shift %= LANES
    return pltpu.roll(value, shift, 1) if shift else value


def depth_kernel(flags, x_ref, t1, t2, t3, from_lo, from_hi, t1_out, t2_out, t3_out, lo_out, hi_out):
    lane = lanes()
    low = jnp.where(flags[4] > 0, from_lo[...].astype(F32), 0.0)
    high = jnp.where(flags[5] > 0, from_hi[...].astype(F32), 0.0)

    def joined(own, mask_lo, shift_lo, mask_hi, shift_hi):
        value = own.astype(F32)
        value = jnp.where(mask_lo, rolled(low, shift_lo), value)
        return jnp.where(mask_hi, rolled(high, shift_hi), value)

    extra = []
    for x in range(2):
        for y in range(2):
            tile = 2 * x + y
            value = joined(
                t2[x, y], lane < 2, 32 - 2 * tile, (lane >= 34) & (lane < 36), 34 - 96 - 2 * tile
            )
            t2_out[x, y] = value.astype(BF16)
            extra.append(rolled(value, 72))
    value = joined(t3[...], lane < 2, 24, (lane >= 18) & (lane < 20), 18 - 104)
    t3_out[...] = value.astype(BF16)
    extra.append(rolled(value, 72))
    free = (lane >= 72) & (lane < 108)
    mask_lo = (lane >= 124) | (lane < 2)
    mask_hi = (lane >= 66) & (lane < 72)
    for x in range(4):
        for y in range(4):
            tile = 4 * x + y
            value = joined(t1[x, y], mask_lo, 124 - 6 * tile, mask_hi, 66 - 6 * tile)
            t1_out[x, y] = value.astype(BF16)
            k = tile % 8
            if k < 5:
                value = jnp.where(free, extra[k], value)
            (lo_out if x < 2 else hi_out)[8 + k] = value.astype(BF16)
    lo_out[0:8] = x_ref[0]
    hi_out[0:8] = x_ref[7]


def kept(flag, value):
    return jnp.where(flag > 0, value, jnp.zeros_like(value))


def width_kernel(flags, x_ref, t1, t2, t3, xr_lo, xr_hi, xr_lo2, xr_hi2, lo_out, hi_out, two_out):
    has_lo, has_hi, has_lo2, has_hi2 = flags[0], flags[1], flags[6], flags[7]
    lane = lanes()
    free = (lane >= 72) & (lane < 124)
    row = [
        rolled(kept(has_lo2, xr_lo2[...]).astype(F32), 0),
        rolled(kept(has_lo, xr_lo[12]).astype(F32), -72),
        t3[...].astype(F32),
        rolled(kept(has_hi, xr_hi[12]).astype(F32), -72),
        rolled(kept(has_hi2, xr_hi2[...]).astype(F32), 0),
    ]
    two = row[0]
    for i in range(1, 5):
        two = jnp.where(lane < 20 * i, two, rolled(row[i], 20 * i))
    two_out[...] = two.astype(BF16)
    coarse = [rolled(two, 72), rolled(two, 72 - 40), rolled(two, 72 - 80)]

    for out, fine_y, half_y in ((lo_out, 0, 0), (hi_out, 7, 2)):
        out[0] = kept(has_lo, xr_lo[fine_y])
        out[9] = kept(has_hi, xr_hi[fine_y])
        for x in range(8):
            out[1 + x] = x_ref[x, fine_y]
        for i in range(8):
            for k in range(2):
                y = half_y + k
                if i < 2:
                    value = kept(has_lo, xr_lo[8 + 4 * i + y])
                elif i < 6:
                    value = t1[i - 2, y]
                else:
                    value = kept(has_hi, xr_hi[8 + 4 * (i - 6) + y])
                if i < 2:
                    extra = kept(has_lo, xr_lo[8 + 2 * i + k]).astype(F32)
                elif i < 4:
                    extra = rolled(t2[i - 2, k].astype(F32), 72)
                elif i < 6:
                    extra = kept(has_hi, xr_hi[8 + 2 * (i - 4) + k]).astype(F32)
                else:
                    spot = 2 * (i - 6) + k
                    extra = coarse[spot] if spot < 3 else None
                if extra is not None:
                    value = jnp.where(free, extra, value.astype(F32)).astype(BF16)
                out[10 + 2 * i + k] = value


def taps(ref, x, ys):
    return jnp.concatenate(
        [
            jnp.concatenate([ref[x + d, y : y + 3].reshape(288, LANES) for y in ys], axis=1)
            for d in range(3)
        ],
        axis=0,
    )


def weighted(weight, value):
    return lax.dot_general(weight, value, (((0,), (0,)), ((), ())), preferred_element_type=F32)


def spread(ref, i, j, value, base=0, lo=None, hi=None):
    lane = lanes()
    wide = value.astype(F32)
    before, after = rolled(wide, base + 1), rolled(wide, base - 1)
    if lo is not None:
        before = jnp.where(lane == 0, lo, before)
        after = jnp.where(lane == LANES - 1, hi, after)
    ref[i, j, 0:32] = before.astype(BF16)
    ref[i, j, 32:64] = rolled(wide, base).astype(BF16) if base else value
    ref[i, j, 64:96] = after.astype(BF16)


def fine_kernel(flags, x_ref, t1, xr_lo, xr_hi, w0, mix, acc_out, e0):
    zero = jnp.zeros((96, LANES), BF16)
    for i in range(10):
        e0[i, 0] = zero
        e0[i, 9] = zero
    for k in range(8):
        s = k % 2
        column = kept(flags[0], xr_lo[8 + 4 + k // 2]).astype(F32)
        spread(e0, 0, 1 + k, kept(flags[0], xr_lo[k]), 0, rolled(column, 2 - s), rolled(column, 57 - s))
        column = kept(flags[1], xr_hi[8 + k // 2]).astype(F32)
        spread(e0, 9, 1 + k, kept(flags[1], xr_hi[k]), 0, rolled(column, 4 - s), rolled(column, 59 - s))

    def fill(c, carry):
        for part in range(2):
            for k in range(8):
                s = 2 * part + k % 2
                column = t1[c, k // 2].astype(F32)
                spread(
                    e0, 2 * c + part + 1, 1 + k, x_ref[2 * c + part, k], 0,
                    rolled(column, 4 - s), rolled(column, 59 - s),
                )
        return carry

    lax.fori_loop(0, 4, fill, 0)
    weight = jnp.concatenate([w0[...], mix[...]], axis=0)

    def fine(x, carry):
        for y in range(0, 8, 2):
            middle = jnp.concatenate([x_ref[x, y], x_ref[x, y + 1]], axis=1)
            value = weighted(weight, jnp.concatenate([taps(e0, x, [y, y + 1]), middle], axis=0))
            acc_out[x, y] = value[:, :LANES]
            acc_out[x, y + 1] = value[:, LANES:]
        return carry

    lax.fori_loop(0, 8, fine, 0)


def final_kernel(
    flags, acc, t1, t2, t3, xr_lo, xr_hi, xr_lo2, xr_hi2, yr_lo, yr_hi, yr_two,
    w0, w1, w2, w3, up, up0, out_ref, ey, edge, e1, e2, e3, v3, v2, v1, q1, rows,
):
    x_lo, x_hi, y_lo, y_hi, z_lo, z_hi, x_lo2, x_hi2, y_lo2, y_hi2 = (flags[i] for i in range(10))
    lane = lanes()

    for i in range(5):
        spread(e3, i, 0, kept(y_lo2, yr_two[...]), -20 * i)
        spread(e3, i, 1, kept(y_lo, yr_lo[22 + i // 2]), -72 - 20 * (i % 2))
        spread(e3, i, 3, kept(y_hi, yr_hi[22 + i // 2]), -72 - 20 * (i % 2))
        spread(e3, i, 4, kept(y_hi2, yr_two[...]), -20 * i)
    spread(e3, 0, 2, kept(x_lo2, xr_lo2[...]))
    spread(e3, 1, 2, kept(x_lo, xr_lo[12]), -72)
    spread(e3, 2, 2, t3[...])
    spread(e3, 3, 2, kept(x_hi, xr_hi[12]), -72)
    spread(e3, 4, 2, kept(x_hi2, xr_hi2[...]))
    for i in range(6):
        for k in range(2):
            spread(e2, i, k, kept(y_lo, yr_lo[10 + 2 * i + k]), -72)
            spread(e2, i, 4 + k, kept(y_hi, yr_hi[10 + 2 * i + k]), -72)
    for i in range(2):
        for k in range(2):
            spread(e2, i, 2 + k, kept(x_lo, xr_lo[8 + 2 * i + k]), -72)
            spread(e2, 2 + i, 2 + k, t2[i, k])
            spread(e2, 4 + i, 2 + k, kept(x_hi, xr_hi[8 + 2 * i + k]), -72)
    for i in range(8):
        for k in range(2):
            spread(e1, i, k, kept(y_lo, yr_lo[10 + 2 * i + k]))
            spread(e1, i, 6 + k, kept(y_hi, yr_hi[10 + 2 * i + k]))
    for k in range(4):
        for i in range(2):
            spread(e1, i, 2 + k, kept(x_lo, xr_lo[8 + 4 * i + k]))
            spread(e1, 6 + i, 2 + k, kept(x_hi, xr_hi[8 + 4 * i + k]))
        for i in range(4):
            spread(e1, 2 + i, 2 + k, t1[i, k])
    for i in range(10):
        sx = (i + 1) % 2
        coarse = (i + 1) // 2 + 1
        for side, ref, flag, row, s in ((0, yr_lo, y_lo, 1, 2 * sx + 1), (1, yr_hi, y_hi, 0, 2 * sx)):
            column = kept(flag, ref[10 + 2 * coarse + row]).astype(F32)
            spread(ey, side, i, kept(flag, ref[i]), 0, rolled(column, 4 - s), rolled(column, 59 - s))
    for side, dy in ((0, 0), (1, 2)):
        weight = jnp.concatenate([w0[96 * (3 * dx + dy) : 96 * (3 * dx + dy) + 96] for dx in range(3)], axis=0)
        for x in range(0, 8, 2):
            value = jnp.concatenate(
                [ey[side, x : x + 3].reshape(288, LANES), ey[side, x + 1 : x + 4].reshape(288, LANES)], axis=1
            )
            value = weighted(weight, value)
            edge[side, x] = value[:, :LANES]
            edge[side, x + 1] = value[:, LANES:]

    def along(before, centre, after):
        return [0.75 * centre + 0.25 * before, 0.75 * centre + 0.25 * after]

    def limits(count):
        inside = (lane >= 1) & (lane <= count + 2)
        inside &= (lane != 1) | (z_lo > 0)
        return inside & ((lane != count + 2) | (z_hi > 0))

    def cell_flag(position, last, lo, hi):
        return lo if position == 0 else hi if position == last else None

    def prolonged(ref, count):
        wide = dot(ref[...].reshape(count * count * 32, LANES), up[...]).reshape(count, count, 32, LANES)

        def refined(cells):
            out = []
            for k in range(2 * count - 2):
                cell = k - 1
                centre = cell // 2 + 1
                other = centre - 1 if cell % 2 == 0 else centre + 1
                out.append(0.75 * cells[centre] + 0.25 * cells[other])
            return out

        by_x = refined([wide[i] for i in range(count)])
        return [refined([row[j] for j in range(count)]) for row in by_x]

    def level(e_ref, w_ref, v_ref, size, cells, above):
        keep = limits(cells)
        for i in range(size):
            for j in range(0, size, 2):
                ys = [j, j + 1] if j + 1 < size else [j]
                value = weighted(w_ref[...], taps(e_ref, i, ys))
                for n, y in enumerate(ys):
                    part = value[:, LANES * n : LANES * (n + 1)]
                    if above is not None:
                        part = part + above[i][y]
                    good = keep
                    for flag in (cell_flag(i, size - 1, x_lo, x_hi), cell_flag(y, size - 1, y_lo, y_hi)):
                        if flag is not None:
                            good = good & (flag > 0)
                    v_ref[i, y] = jnp.where(good, part, 0.0).astype(BF16)

    level(e3, w3, v3, 3, 16, None)
    level(e2, w2, v2, 4, 32, prolonged(v3, 3))
    level(e1, w1, v1, 6, 64, prolonged(v2, 4))
    for i in range(6):
        q1[i] = dot(v1[i].reshape(6 * 32, LANES), up0[...]).reshape(6, 32, LANES)

    def fine(c, carry):
        for part in range(2):
            x = 2 * c + part
            row = 0.75 * q1[c + 1] + 0.25 * q1[c + 2 * part]
            for y in range(0, 8, 2):
                centre = y // 2 + 1
                for n, extra in enumerate(along(row[centre - 1], row[centre], row[centre + 1])):
                    total = acc[x, y + n] + extra
                    if y + n == 0:
                        total = total + edge[0, x]
                    if y + n == 7:
                        total = total + edge[1, x]
                    rows[pl.ds(x * 8 + y + n, 32, stride=64), :] = jax.nn.gelu(total, approximate=True)
        return carry

    lax.fori_loop(0, 4, fine, 0)
    out_ref[...] = rows[...].reshape(32, 8, 8, LANES).astype(BF16)


def turned(value, axis, step):
    count = lax.axis_size(axis)
    return lax.ppermute(value, axis, [(i, (i + step) % count) for i in range(count)])


def on_device(field, mixing, kernel_fine, kernel_half, kernel_quarter, kernel_eighth):
    gx, gy, gz = (lax.axis_index(a) for a in ("gx", "gy", "gz"))
    nx, ny, nz = (lax.axis_size(a) for a in ("gx", "gy", "gz"))
    slot = lax.iota(jnp.int32, 16)
    place = jnp.where((slot < 2) | (slot == 6) | (slot == 7), gx, jnp.where((slot == 4) | (slot == 5), gz, gy))
    side = slot & 1
    width = jnp.where(slot < 6, 1, 2)
    count = jnp.where((slot < 2) | (slot == 6) | (slot == 7), nx, jnp.where((slot == 4) | (slot == 5), nz, ny))
    flags = jnp.where(side == 0, place >= width, place < count - width).astype(jnp.int32)
    up, up0 = (jnp.asarray(m) for m in tables())
    tile = (32, LANES)

    (table,) = call(restrictions, [(512, 640)], [], scalars=0, flops=1 << 26)
    x_own, t1, t2, t3, msg = call(
        restrict_kernel,
        [(8, 8) + tile, (4, 4) + tile, (2, 2) + tile, tile, (2,) + tile],
        [field, table],
        [pltpu.VMEM((2048, LANES), F32)],
        0,
    )
    from_hi = turned(msg[0], "gz", -1)
    from_lo = turned(msg[1], "gz", 1)
    t1, t2, t3, x_msg_lo, x_msg_hi = call(
        depth_kernel,
        [(4, 4) + tile, (2, 2) + tile, tile, (16,) + tile, (16,) + tile],
        [flags, x_own, t1, t2, t3, from_lo, from_hi],
    )
    xr_hi = turned(x_msg_lo, "gx", -1)
    xr_lo = turned(x_msg_hi, "gx", 1)
    xr_hi2 = turned(t3, "gx", -2)
    xr_lo2 = turned(t3, "gx", 2)
    y_msg_lo, y_msg_hi, two = call(
        width_kernel,
        [(26,) + tile, (26,) + tile, tile],
        [flags, x_own, t1, t2, t3, xr_lo, xr_hi, xr_lo2, xr_hi2],
    )
    yr_hi = turned(y_msg_lo, "gy", -1)
    yr_lo = turned(y_msg_hi, "gy", 1)
    assert ny == 4
    yr_two = turned(two, "gy", 2)
    flat = [k.reshape(864, 32) for k in (kernel_fine, kernel_half, kernel_quarter, kernel_eighth)]
    (acc,) = call(
        fine_kernel,
        [(8, 8) + tile],
        [flags, x_own, t1, xr_lo, xr_hi, flat[0], mixing.T],
        [pltpu.VMEM((10, 10, 96, LANES), BF16)],
        kind=F32,
        flops=1 << 30,
    )
    (out,) = call(
        final_kernel,
        [(32, 8, 8, LANES)],
        [flags, acc, t1, t2, t3, xr_lo, xr_hi, xr_lo2, xr_hi2, yr_lo, yr_hi, yr_two,
         *flat, up, up0],
        [
            pltpu.VMEM((2, 10, 96, LANES), BF16),
            pltpu.VMEM((2, 8) + tile, F32),
            pltpu.VMEM((8, 8, 96, LANES), BF16),
            pltpu.VMEM((6, 6, 96, LANES), BF16),
            pltpu.VMEM((5, 5, 96, LANES), BF16),
            pltpu.VMEM((3, 3) + tile, BF16),
            pltpu.VMEM((4, 4) + tile, BF16),
            pltpu.VMEM((6, 6) + tile, BF16),
            pltpu.VMEM((6, 6) + tile, F32),
            pltpu.VMEM((2048, LANES), F32),
        ],
    )
    return out


def solution(mesh):
    placed = (P(None, "gx", "gy", "gz"), P(), P(), P(), P(), P())
    return jax.shard_map(
        on_device, mesh=mesh, in_specs=placed, out_specs=P(None, "gx", "gy", "gz"), check_vma=False
    )
```

```python
import jax
import jax.numpy as jnp
import numpy as np
from jax import lax
from jax.experimental import pallas as pl
from jax.experimental.pallas import tpu as pltpu
from jax.sharding import PartitionSpec as P


INTERPRET = False
F32, BF16 = jnp.float32, jnp.bfloat16
LANES = 128
GROUP = 4


def tables():
    up = np.zeros((128, 128), np.float32)
    up0 = np.zeros((128, 128), np.float32)
    for out in range(128):
        step = -1 if out % 2 == 0 else 1
        centre = out // 2 + 1
        if 0 <= centre + step:
            up[centre, out] += 0.75
            up[centre + step, out] += 0.25
        centre = out // 2 + 2
        up0[centre, out] += 0.75
        up0[centre + step, out] += 0.25
    return tuple(m.astype(BF16) for m in (up, up0))


def restrictions(table):
    row = lax.broadcasted_iota(jnp.int32, (512, LANES), 0)
    lane = lax.broadcasted_iota(jnp.int32, (1, LANES), 1)
    spot = row & 127
    eighth = jnp.float32(0.125)

    def put(k, *terms):
        value = jnp.zeros((512, LANES), F32)
        for mask, amount in terms:
            value = jnp.where(mask, amount, value)
        table[:, LANES * k : LANES * (k + 1)] = value.astype(BF16)

    def at(target, valid):
        return row == jnp.where(valid, target, -1)

    put(
        0,
        ((spot >> 1) + 2 == lane, eighth),
        (at((lane - 72) * 128, (lane >= 72) & (lane < 76)), 1.0),
        (at((lane - 76) * 128 + 127, (lane >= 76) & (lane < 80)), 1.0),
    )
    halves = ((spot - 2) >> 1) + 2 == lane
    sub = ((lane - 40) * 43) >> 8
    k = lane - 40 - 6 * sub
    low = at(sub * 128 + jnp.where(k < 2, 2 + k, 70 + k), (lane >= 40) & (lane < 64))
    sub = ((lane - 64) * 43) >> 8
    k = lane - 64 - 6 * sub
    high = at(sub * 128 + jnp.where(k < 4, 76 + k, 60 + k), (lane >= 64) & (lane < 88))
    put(1, (halves & (spot < 66) & (spot >= 2), eighth), (low, 1.0), (high, 1.0))
    put(2, (halves & (spot < 34) & (spot >= 2), eighth))
    tile = (lane * 43) >> 8
    k = lane - 6 * tile
    quad = (tile >> 3) * 2 + ((tile & 3) >> 1)
    sub = ((tile >> 2) & 1) * 2 + (tile & 1)
    last = (lane - 104) * 2
    for n, start, own, own3 in ((3, 40, 2, 2), (4, 64, 32, 30)):
        target = jnp.where(lane < 96, quad * 128 + start + 6 * sub + k, ((lane - 96) >> 1) * 128 + own + (lane & 1))
        tail = ((spot - own3) & ~1) == jnp.where((lane >= 104) & (lane < 106), last, -1000)
        put(n, (at(target, lane < 104), 1.0), (tail, eighth))


def dot(a, b):
    return jnp.dot(a, b, preferred_element_type=F32)


def call(kernel, outs, args, scratch=(), scalars=1, kind=BF16, flops=1 << 20):
    specs = [pl.BlockSpec(memory_space=pltpu.SMEM)] * scalars
    specs += [pl.BlockSpec(memory_space=pltpu.VMEM)] * (len(args) - scalars)
    return pl.pallas_call(
        kernel,
        out_shape=[jax.ShapeDtypeStruct(shape, kind) for shape in outs],
        in_specs=specs,
        out_specs=[pl.BlockSpec(memory_space=pltpu.VMEM)] * len(outs),
        scratch_shapes=list(scratch),
        compiler_params=pltpu.CompilerParams(vmem_limit_bytes=48 * 1024 * 1024),
        cost_estimate=pl.CostEstimate(flops=flops, transcendentals=0, bytes_accessed=1 << 20),
        interpret=INTERPRET,
    )(*args)


def restrict_kernel(field, table, x_out, t1_out, t2_out, t3_out, msg_out, rows):
    rows[...] = field[...].astype(F32).reshape(2048, LANES)
    for x in range(8):
        for y in range(8):
            x_out[x, y] = rows[pl.ds(x * 8 + y, 32, stride=64), :].astype(BF16)

    def four(ref, x, y):
        return jnp.concatenate(
            [ref[2 * x, 2 * y], ref[2 * x, 2 * y + 1], ref[2 * x + 1, 2 * y], ref[2 * x + 1, 2 * y + 1]],
            axis=1,
        )

    for x in range(4):
        left = jnp.concatenate([four(x_out, x, y) for y in range(4)], axis=0)
        t1_out[x] = dot(left, table[:, 0:128]).astype(BF16).reshape(4, 32, LANES)
    left = jnp.concatenate([four(t1_out, x, y) for x in range(2) for y in range(2)], axis=0)
    t2_out[...] = dot(left, table[:, 128:256]).astype(BF16).reshape(2, 2, 32, LANES)
    t3 = dot(four(t2_out, 0, 0), table[:, 256:640]).astype(BF16)
    t3_out[...] = t3[:, :128]
    msg_out[0] = t3[:, 128:256]
    msg_out[1] = t3[:, 256:]


def lanes():
    return lax.broadcasted_iota(jnp.int32, (32, LANES), 1)


def rolled(value, shift):
    shift %= LANES
    return pltpu.roll(value, shift, 1) if shift else value


def depth_kernel(flags, x_ref, t1, t2, t3, from_lo, from_hi, t1_out, t2_out, t3_out, lo_out, hi_out):
    lane = lanes()
    low = jnp.where(flags[4] > 0, from_lo[...].astype(F32), 0.0)
    high = jnp.where(flags[5] > 0, from_hi[...].astype(F32), 0.0)

    def joined(own, mask_lo, shift_lo, mask_hi, shift_hi):
        value = own.astype(F32)
        value = jnp.where(mask_lo, rolled(low, shift_lo), value)
        return jnp.where(mask_hi, rolled(high, shift_hi), value)

    extra = []
    for x in range(2):
        for y in range(2):
            tile = 2 * x + y
            value = joined(
                t2[x, y], lane < 2, 32 - 2 * tile, (lane >= 34) & (lane < 36), 34 - 96 - 2 * tile
            )
            t2_out[x, y] = value.astype(BF16)
            extra.append(rolled(value, 72))
    value = joined(t3[...], lane < 2, 24, (lane >= 18) & (lane < 20), 18 - 104)
    t3_out[...] = value.astype(BF16)
    extra.append(rolled(value, 72))
    free = (lane >= 72) & (lane < 108)
    mask_lo = (lane >= 124) | (lane < 2)
    mask_hi = (lane >= 66) & (lane < 72)
    for x in range(4):
        for y in range(4):
            tile = 4 * x + y
            value = joined(t1[x, y], mask_lo, 124 - 6 * tile, mask_hi, 66 - 6 * tile)
            t1_out[x, y] = value.astype(BF16)
            k = tile % 8
            if k < 5:
                value = jnp.where(free, extra[k], value)
            (lo_out if x < 2 else hi_out)[8 + k] = value.astype(BF16)
    lo_out[0:8] = x_ref[0]
    hi_out[0:8] = x_ref[7]


def kept(flag, value):
    return jnp.where(flag > 0, value, jnp.zeros_like(value))


def width_kernel(flags, x_ref, t1, t2, t3, xr_lo, xr_hi, xr_lo2, xr_hi2, lo_out, hi_out, two_out):
    has_lo, has_hi, has_lo2, has_hi2 = flags[0], flags[1], flags[6], flags[7]
    lane = lanes()
    free = (lane >= 72) & (lane < 124)
    row = [
        rolled(kept(has_lo2, xr_lo2[...]).astype(F32), 0),
        rolled(kept(has_lo, xr_lo[12]).astype(F32), -72),
        t3[...].astype(F32),
        rolled(kept(has_hi, xr_hi[12]).astype(F32), -72),
        rolled(kept(has_hi2, xr_hi2[...]).astype(F32), 0),
    ]
    two = row[0]
    for i in range(1, 5):
        two = jnp.where(lane < 20 * i, two, rolled(row[i], 20 * i))
    two_out[...] = two.astype(BF16)
    coarse = [rolled(two, 72), rolled(two, 72 - 40), rolled(two, 72 - 80)]

    for out, fine_y, half_y in ((lo_out, 0, 0), (hi_out, 7, 2)):
        out[0] = kept(has_lo, xr_lo[fine_y])
        out[9] = kept(has_hi, xr_hi[fine_y])
        for x in range(8):
            out[1 + x] = x_ref[x, fine_y]
        for i in range(8):
            for k in range(2):
                y = half_y + k
                if i < 2:
                    value = kept(has_lo, xr_lo[8 + 4 * i + y])
                elif i < 6:
                    value = t1[i - 2, y]
                else:
                    value = kept(has_hi, xr_hi[8 + 4 * (i - 6) + y])
                if i < 2:
                    extra = kept(has_lo, xr_lo[8 + 2 * i + k]).astype(F32)
                elif i < 4:
                    extra = rolled(t2[i - 2, k].astype(F32), 72)
                elif i < 6:
                    extra = kept(has_hi, xr_hi[8 + 2 * (i - 4) + k]).astype(F32)
                else:
                    spot = 2 * (i - 6) + k
                    extra = coarse[spot] if spot < 3 else None
                if extra is not None:
                    value = jnp.where(free, extra, value.astype(F32)).astype(BF16)
                out[10 + 2 * i + k] = value


def weighted(weight, value):
    return lax.dot_general(weight, value, (((0,), (0,)), ((), ())), preferred_element_type=F32)


def spread(ref, i, j, value, base=0, lo=None, hi=None):
    lane = lanes()
    wide = value.astype(F32)
    before, after = rolled(wide, base + 1), rolled(wide, base - 1)
    if lo is not None:
        before = jnp.where(lane == 0, lo, before)
        after = jnp.where(lane == LANES - 1, hi, after)
    ref[i, j, 0:32] = before.astype(BF16)
    ref[i, j, 32:64] = rolled(wide, base).astype(BF16) if base else value
    ref[i, j, 64:96] = after.astype(BF16)


def block(w, dz):
    return jnp.concatenate([w[96 * k + 32 * dz : 96 * k + 32 * dz + 32] for k in range(9)], axis=0)


def weights_kernel(w0, w1, w2, w3, mix, f_out, a1_out, a2_out, a3_out):
    row = lax.broadcasted_iota(jnp.int32, (32, 96), 0)
    column = lax.broadcasted_iota(jnp.int32, (32, 96), 1)
    spots = [jnp.where(column == row + 32 * dz, 1.0, 0.0).astype(BF16) for dz in range(3)]

    def placed(dz, value):
        return lax.dot_general(spots[dz], value, (((0,), (1,)), ((), ())), preferred_element_type=F32)

    for w, out in ((w0, f_out), (w1, a1_out), (w2, a2_out), (w3, a3_out)):
        total = placed(0, block(w, 0)) + placed(1, block(w, 1)) + placed(2, block(w, 2))
        out[:, 0:288] = total.astype(BF16)
    mixed = lax.dot_general(spots[1], mix[...], (((0,), (0,)), ((), ())), preferred_element_type=F32)
    f_out[:, 288:320] = mixed.astype(BF16)


def around(ref, x, ys):
    return jnp.concatenate(
        [jnp.concatenate([ref[x + d, y : y + 3].reshape(96, LANES) for y in ys], axis=1) for d in range(3)],
        axis=0,
    )


def shifted(value, n, lo=None, hi=None):
    part = value[:, LANES * n : LANES * (n + 1)]
    before, after = rolled(part[0:32], 1), rolled(part[64:96], -1)
    if lo is not None:
        lane = lanes()
        before = jnp.where(lane == 0, lo, before)
        after = jnp.where(lane == LANES - 1, hi, after)
    return part[32:64] + before + after


def fine_kernel(x_ref, t1, w0, wf, acc_out, f0):
    lane = lanes()
    zero = jnp.zeros((32, LANES), BF16)
    for i in range(10):
        f0[i, 0] = zero
        f0[i, 9] = zero
        f0[0, i] = zero
        f0[9, i] = zero
    f0[1:9, 1:9] = x_ref[...]
    low = jnp.zeros((32, LANES), F32)
    high = jnp.zeros((32, LANES), F32)
    for i in range(4):
        for j in range(4):
            value = t1[i, j].astype(F32)
            for sx in range(2):
                spot = 12 * (2 * i + sx + 1) + 2 * j + 1
                here = (lane >= spot) & (lane < spot + 2)
                low = jnp.where(here, rolled(value, spot - 124 - 2 * sx), low)
                high = jnp.where(here, rolled(value, spot - 68 - 2 * sx), high)

    def columns(value, dz):
        near = [rolled(value, -12 * dx - dy).astype(BF16) for dx in (-1, 0, 1) for dy in (-1, 0, 1)]
        return weighted(block(w0, dz), jnp.concatenate(near, axis=0))

    low, high = columns(low, 0), columns(high, 2)
    for x in range(8):
        for y in range(0, 8, GROUP):
            ys = range(y, y + GROUP)
            middle = jnp.concatenate([x_ref[x, k] for k in ys], axis=1)
            value = dot(wf[...], jnp.concatenate([around(f0, x, ys), middle], axis=0))
            for n, k in enumerate(ys):
                spot = 12 * (x + 1) + k + 1
                acc_out[x, k] = shifted(value, n, rolled(low, -spot), rolled(high, 127 - spot))


def own_rows_kernel(
    flags, t1, t2, t3, xr_lo, xr_hi, xr_lo2, xr_hi2, w0, wf1, wf2, wf3,
    edge_out, a1_out, a2_out, a3_out, ex, f1, f2, f3,
):
    x_lo, x_hi, x_lo2, x_hi2 = flags[0], flags[1], flags[6], flags[7]
    zero = jnp.zeros((32, LANES), BF16)
    for ref, size in ((f1, 6), (f2, 4), (f3, 3)):
        for i in range(size + 2):
            for j in (0, 1, size, size + 1):
                ref[i, j] = zero
    for side in range(2):
        for j in (0, 9):
            ex[side, j] = jnp.zeros((96, LANES), BF16)
    for k in range(8):
        s = k % 2
        column = kept(x_lo, xr_lo[8 + 4 + k // 2]).astype(F32)
        spread(ex, 0, 1 + k, kept(x_lo, xr_lo[k]), 0, rolled(column, 2 - s), rolled(column, 57 - s))
        column = kept(x_hi, xr_hi[8 + k // 2]).astype(F32)
        spread(ex, 1, 1 + k, kept(x_hi, xr_hi[k]), 0, rolled(column, 4 - s), rolled(column, 59 - s))

    def back(value):
        return rolled(value.astype(F32), -72).astype(BF16)

    for k in range(4):
        for i in range(2):
            f1[i, 2 + k] = kept(x_lo, xr_lo[8 + 4 * i + k])
            f1[6 + i, 2 + k] = kept(x_hi, xr_hi[8 + 4 * i + k])
        for i in range(4):
            f1[2 + i, 2 + k] = t1[i, k]
    for i in range(2):
        for k in range(2):
            f2[i, 2 + k] = back(kept(x_lo, xr_lo[8 + 2 * i + k]))
            f2[2 + i, 2 + k] = t2[i, k]
            f2[4 + i, 2 + k] = back(kept(x_hi, xr_hi[8 + 2 * i + k]))
    f3[0, 2] = kept(x_lo2, xr_lo2[...])
    f3[1, 2] = back(kept(x_lo, xr_lo[12]))
    f3[2, 2] = t3[...]
    f3[3, 2] = back(kept(x_hi, xr_hi[12]))
    f3[4, 2] = kept(x_hi2, xr_hi2[...])

    for side, dx in ((0, 0), (1, 2)):
        weight = w0[288 * dx : 288 * dx + 288]
        for y in range(0, 8, 2):
            value = jnp.concatenate(
                [ex[side, y : y + 3].reshape(288, LANES), ex[side, y + 1 : y + 4].reshape(288, LANES)], axis=1
            )
            value = weighted(weight, value)
            edge_out[side, y] = value[:, :LANES]
            edge_out[side, y + 1] = value[:, LANES:]
    for ref, w, out, size in ((f3, wf3, a3_out, 3), (f2, wf2, a2_out, 4), (f1, wf1, a1_out, 6)):
        for i in range(size):
            value = dot(w[...], around(ref, i, range(size)))
            for j in range(size):
                out[i, j] = shifted(value, j)


def final_kernel(
    flags, acc, edge_x, a1, a2, a3, yr_lo, yr_hi, yr_two,
    w0, w1, w2, w3, up, up0, out_ref, ey, edge, e1, e2, e3, v3, v2, v1, q1, rows,
):
    x_lo, x_hi, y_lo, y_hi, z_lo, z_hi = (flags[i] for i in range(6))
    y_lo2, y_hi2 = flags[8], flags[9]
    lane = lanes()

    for i in range(5):
        spread(e3, i, 0, kept(y_lo2, yr_two[...]), -20 * i)
        spread(e3, i, 1, kept(y_lo, yr_lo[22 + i // 2]), -72 - 20 * (i % 2))
        spread(e3, i, 3, kept(y_hi, yr_hi[22 + i // 2]), -72 - 20 * (i % 2))
        spread(e3, i, 4, kept(y_hi2, yr_two[...]), -20 * i)
    for i in range(6):
        for k in range(2):
            spread(e2, i, k, kept(y_lo, yr_lo[10 + 2 * i + k]), -72)
            spread(e2, i, 4 + k, kept(y_hi, yr_hi[10 + 2 * i + k]), -72)
    for i in range(8):
        for k in range(2):
            spread(e1, i, k, kept(y_lo, yr_lo[10 + 2 * i + k]))
            spread(e1, i, 6 + k, kept(y_hi, yr_hi[10 + 2 * i + k]))
    for i in range(10):
        sx = (i + 1) % 2
        coarse = (i + 1) // 2 + 1
        for side, ref, flag, row, s in ((0, yr_lo, y_lo, 1, 2 * sx + 1), (1, yr_hi, y_hi, 0, 2 * sx)):
            column = kept(flag, ref[10 + 2 * coarse + row]).astype(F32)
            spread(ey, side, i, kept(flag, ref[i]), 0, rolled(column, 4 - s), rolled(column, 59 - s))
    for side, dy in ((0, 0), (1, 2)):
        weight = jnp.concatenate([w0[96 * (3 * dx + dy) : 96 * (3 * dx + dy) + 96] for dx in range(3)], axis=0)
        for x in range(0, 8, 2):
            value = jnp.concatenate(
                [ey[side, x : x + 3].reshape(288, LANES), ey[side, x + 1 : x + 4].reshape(288, LANES)], axis=1
            )
            value = weighted(weight, value)
            edge[side, x] = value[:, :LANES]
            edge[side, x + 1] = value[:, LANES:]

    def along(before, centre, after):
        return [0.75 * centre + 0.25 * before, 0.75 * centre + 0.25 * after]

    def limits(count):
        inside = (lane >= 1) & (lane <= count + 2)
        inside &= (lane != 1) | (z_lo > 0)
        return inside & ((lane != count + 2) | (z_hi > 0))

    def cell_flag(position, last, lo, hi):
        return lo if position == 0 else hi if position == last else None

    def prolonged(ref, count):
        wide = dot(ref[...].reshape(count * count * 32, LANES), up[...]).reshape(count, count, 32, LANES)

        def refined(cells):
            out = []
            for k in range(2 * count - 2):
                cell = k - 1
                centre = cell // 2 + 1
                other = centre - 1 if cell % 2 == 0 else centre + 1
                out.append(0.75 * cells[centre] + 0.25 * cells[other])
            return out

        by_x = refined([wide[i] for i in range(count)])
        return [refined([row[j] for j in range(count)]) for row in by_x]

    def level(e_ref, w_ref, own, v_ref, size, cells, above):
        keep = limits(cells)
        for j in range(size):
            dys = [dy for dy in range(3) if not 2 <= j + dy < size]
            weight = jnp.concatenate(
                [w_ref[96 * (3 * dx + dy) : 96 * (3 * dx + dy) + 96] for dx in range(3) for dy in dys], axis=0
            ) if dys else None
            for i in range(0, size, 2):
                xs = [i, i + 1] if i + 1 < size else [i]
                if dys:
                    value = jnp.concatenate(
                        [
                            jnp.concatenate([e_ref[x + dx, j + dy] for x in xs], axis=1)
                            for dx in range(3)
                            for dy in dys
                        ],
                        axis=0,
                    )
                    value = weighted(weight, value)
                for n, x in enumerate(xs):
                    part = own[x, j]
                    if dys:
                        part = part + value[:, LANES * n : LANES * (n + 1)]
                    if above is not None:
                        part = part + above[x][j]
                    good = keep
                    for flag in (cell_flag(x, size - 1, x_lo, x_hi), cell_flag(j, size - 1, y_lo, y_hi)):
                        if flag is not None:
                            good = good & (flag > 0)
                    v_ref[x, j] = jnp.where(good, part, 0.0).astype(BF16)

    level(e3, w3, a3, v3, 3, 16, None)
    level(e2, w2, a2, v2, 4, 32, prolonged(v3, 3))
    level(e1, w1, a1, v1, 6, 64, prolonged(v2, 4))
    for i in range(6):
        q1[i] = dot(v1[i].reshape(6 * 32, LANES), up0[...]).reshape(6, 32, LANES)

    def fine(c, side):
        for part in range(2):
            x = 2 * c + part
            row = 0.75 * q1[c + 1] + 0.25 * q1[c + 2 * part]
            for y in range(0, 8, 2):
                centre = y // 2 + 1
                for n, extra in enumerate(along(row[centre - 1], row[centre], row[centre + 1])):
                    total = acc[x, y + n] + extra
                    if y + n == 0:
                        total = total + edge[0, x]
                    if y + n == 7:
                        total = total + edge[1, x]
                    if side == part:
                        total = total + edge_x[side, y + n]
                    rows[pl.ds(x * 8 + y + n, 32, stride=64), :] = jax.nn.gelu(total, approximate=True)

    fine(0, 0)
    lax.fori_loop(1, 3, lambda c, carry: (fine(c, -1), carry)[1], 0)
    fine(3, 1)
    out_ref[...] = rows[...].reshape(32, 8, 8, LANES).astype(BF16)


def turned(value, axis, step):
    count = lax.axis_size(axis)
    return lax.ppermute(value, axis, [(i, (i + step) % count) for i in range(count)])


def on_device(field, mixing, kernel_fine, kernel_half, kernel_quarter, kernel_eighth):
    gx, gy, gz = (lax.axis_index(a) for a in ("gx", "gy", "gz"))
    nx, ny, nz = (lax.axis_size(a) for a in ("gx", "gy", "gz"))
    slot = lax.iota(jnp.int32, 16)
    place = jnp.where((slot < 2) | (slot == 6) | (slot == 7), gx, jnp.where((slot == 4) | (slot == 5), gz, gy))
    side = slot & 1
    width = jnp.where(slot < 6, 1, 2)
    count = jnp.where((slot < 2) | (slot == 6) | (slot == 7), nx, jnp.where((slot == 4) | (slot == 5), nz, ny))
    flags = jnp.where(side == 0, place >= width, place < count - width).astype(jnp.int32)
    up, up0 = (jnp.asarray(m) for m in tables())
    tile = (32, LANES)

    (table,) = call(restrictions, [(512, 640)], [], scalars=0, flops=1 << 26)
    x_own, t1, t2, t3, msg = call(
        restrict_kernel,
        [(8, 8) + tile, (4, 4) + tile, (2, 2) + tile, tile, (2,) + tile],
        [field, table],
        [pltpu.VMEM((2048, LANES), F32)],
        0,
    )
    flat = [k.reshape(864, 32) for k in (kernel_fine, kernel_half, kernel_quarter, kernel_eighth)]
    mixing, *flat, t3 = lax.optimization_barrier((mixing, *flat, t3))
    wf = call(weights_kernel, [(96, 320)] + [(96, 288)] * 3, [*flat, mixing], scalars=0, flops=1 << 28)
    from_hi = turned(msg[0], "gz", -1)
    from_lo = turned(msg[1], "gz", 1)
    from_lo, *wf = lax.optimization_barrier((from_lo, *wf))
    t1, t2, t3, x_msg_lo, x_msg_hi = call(
        depth_kernel,
        [(4, 4) + tile, (2, 2) + tile, tile, (16,) + tile, (16,) + tile],
        [flags, x_own, t1, t2, t3, from_lo, from_hi],
    )
    xr_hi = turned(x_msg_lo, "gx", -1)
    xr_lo = turned(x_msg_hi, "gx", 1)
    xr_hi2 = turned(t3, "gx", -2)
    xr_lo2 = turned(t3, "gx", 2)
    (acc,) = call(
        fine_kernel,
        [(8, 8) + tile],
        [x_own, t1, flat[0], wf[0]],
        [pltpu.VMEM((10, 10) + tile, BF16)],
        0,
        kind=F32,
        flops=1 << 30,
    )
    xr_lo, acc = lax.optimization_barrier((xr_lo, acc))
    y_msg_lo, y_msg_hi, two = call(
        width_kernel,
        [(26,) + tile, (26,) + tile, tile],
        [flags, x_own, t1, t2, t3, xr_lo, xr_hi, xr_lo2, xr_hi2],
    )
    yr_hi = turned(y_msg_lo, "gy", -1)
    yr_lo = turned(y_msg_hi, "gy", 1)
    assert ny == 4
    yr_two = turned(two, "gy", 2)
    edge_x, a1, a2, a3 = call(
        own_rows_kernel,
        [(2, 8) + tile, (6, 6) + tile, (4, 4) + tile, (3, 3) + tile],
        [flags, t1, t2, t3, xr_lo, xr_hi, xr_lo2, xr_hi2, flat[0], *wf[1:]],
        [
            pltpu.VMEM((2, 10, 96, LANES), BF16),
            pltpu.VMEM((8, 8) + tile, BF16),
            pltpu.VMEM((6, 6) + tile, BF16),
            pltpu.VMEM((5, 5) + tile, BF16),
        ],
        kind=F32,
        flops=1 << 30,
    )
    (out,) = call(
        final_kernel,
        [(32, 8, 8, LANES)],
        [flags, acc, edge_x, a1, a2, a3, yr_lo, yr_hi, yr_two, *flat, up, up0],
        [
            pltpu.VMEM((2, 10, 96, LANES), BF16),
            pltpu.VMEM((2, 8) + tile, F32),
            pltpu.VMEM((8, 8, 96, LANES), BF16),
            pltpu.VMEM((6, 6, 96, LANES), BF16),
            pltpu.VMEM((5, 5, 96, LANES), BF16),
            pltpu.VMEM((3, 3) + tile, BF16),
            pltpu.VMEM((4, 4) + tile, BF16),
            pltpu.VMEM((6, 6) + tile, BF16),
            pltpu.VMEM((6, 6) + tile, F32),
            pltpu.VMEM((2048, LANES), F32),
        ],
    )
    return out


def solution(mesh):
    placed = (P(None, "gx", "gy", "gz"), P(), P(), P(), P(), P())

    return jax.shard_map(on_device, mesh=mesh, in_specs=placed, out_specs=P(None, "gx", "gy", "gz"), check_vma=False)
```

```python
import jax
import jax.numpy as jnp
import numpy as np
from jax import lax
from jax.experimental import pallas as pl
from jax.experimental.pallas import tpu as pltpu
from jax.sharding import PartitionSpec as P


INTERPRET = False
F32, BF16 = jnp.float32, jnp.bfloat16
LANES = 128
GROUP = 4


def tables():
    up = np.zeros((128, 128), np.float32)
    up0 = np.zeros((128, 128), np.float32)
    for out in range(128):
        step = -1 if out % 2 == 0 else 1
        centre = out // 2 + 1
        if 0 <= centre + step:
            up[centre, out] += 0.75
            up[centre + step, out] += 0.25
        centre = out // 2 + 2
        up0[centre, out] += 0.75
        up0[centre + step, out] += 0.25
    return tuple(m.astype(BF16) for m in (up, up0))


def restrictions(table):
    row = lax.broadcasted_iota(jnp.int32, (512, LANES), 0)
    lane = lax.broadcasted_iota(jnp.int32, (1, LANES), 1)
    spot = row & 127
    eighth = jnp.float32(0.125)

    def put(k, *terms):
        value = jnp.zeros((512, LANES), F32)
        for mask, amount in terms:
            value = jnp.where(mask, amount, value)
        table[:, LANES * k : LANES * (k + 1)] = value.astype(BF16)

    def at(target, valid):
        return row == jnp.where(valid, target, -1)

    put(
        0,
        ((spot >> 1) + 2 == lane, eighth),
        (at((lane - 72) * 128, (lane >= 72) & (lane < 76)), 1.0),
        (at((lane - 76) * 128 + 127, (lane >= 76) & (lane < 80)), 1.0),
    )
    halves = ((spot - 2) >> 1) + 2 == lane
    sub = ((lane - 40) * 43) >> 8
    k = lane - 40 - 6 * sub
    low = at(sub * 128 + jnp.where(k < 2, 2 + k, 70 + k), (lane >= 40) & (lane < 64))
    sub = ((lane - 64) * 43) >> 8
    k = lane - 64 - 6 * sub
    high = at(sub * 128 + jnp.where(k < 4, 76 + k, 60 + k), (lane >= 64) & (lane < 88))
    put(1, (halves & (spot < 66) & (spot >= 2), eighth), (low, 1.0), (high, 1.0))
    put(2, (halves & (spot < 34) & (spot >= 2), eighth))
    tile = (lane * 43) >> 8
    k = lane - 6 * tile
    quad = (tile >> 3) * 2 + ((tile & 3) >> 1)
    sub = ((tile >> 2) & 1) * 2 + (tile & 1)
    last = (lane - 104) * 2
    for n, start, own, own3 in ((3, 40, 2, 2), (4, 64, 32, 30)):
        target = jnp.where(lane < 96, quad * 128 + start + 6 * sub + k, ((lane - 96) >> 1) * 128 + own + (lane & 1))
        tail = ((spot - own3) & ~1) == jnp.where((lane >= 104) & (lane < 106), last, -1000)
        put(n, (at(target, lane < 104), 1.0), (tail, eighth))


def dot(a, b):
    return jnp.dot(a, b, preferred_element_type=F32)


def call(kernel, outs, args, scratch=(), scalars=1, kind=BF16, flops=1 << 20, out_space=pltpu.VMEM):
    specs = [pl.BlockSpec(memory_space=pltpu.SMEM)] * scalars
    specs += [pl.BlockSpec(memory_space=pltpu.VMEM)] * (len(args) - scalars)
    return pl.pallas_call(
        kernel,
        out_shape=[jax.ShapeDtypeStruct(shape, kind) for shape in outs],
        in_specs=specs,
        out_specs=[pl.BlockSpec(memory_space=out_space)] * len(outs),
        scratch_shapes=list(scratch),
        compiler_params=pltpu.CompilerParams(vmem_limit_bytes=48 * 1024 * 1024),
        cost_estimate=pl.CostEstimate(flops=flops, transcendentals=0, bytes_accessed=1 << 20),
        interpret=INTERPRET,
    )(*args)


def restrict_kernel(field, table, x_out, t1_out, t2_out, t3_out, msg_out, rows):
    rows[...] = field[...].astype(F32).reshape(2048, LANES)
    for x in range(8):
        for y in range(8):
            x_out[x, y] = rows[pl.ds(x * 8 + y, 32, stride=64), :].astype(BF16)

    def four(ref, x, y):
        return jnp.concatenate(
            [ref[2 * x, 2 * y], ref[2 * x, 2 * y + 1], ref[2 * x + 1, 2 * y], ref[2 * x + 1, 2 * y + 1]],
            axis=1,
        )

    for x in range(4):
        left = jnp.concatenate([four(x_out, x, y) for y in range(4)], axis=0)
        t1_out[x] = dot(left, table[:, 0:128]).astype(BF16).reshape(4, 32, LANES)
    left = jnp.concatenate([four(t1_out, x, y) for x in range(2) for y in range(2)], axis=0)
    t2_out[...] = dot(left, table[:, 128:256]).astype(BF16).reshape(2, 2, 32, LANES)
    t3 = dot(four(t2_out, 0, 0), table[:, 256:640]).astype(BF16)
    t3_out[...] = t3[:, :128]
    msg_out[0] = t3[:, 128:256]
    msg_out[1] = t3[:, 256:]


def lanes():
    return lax.broadcasted_iota(jnp.int32, (32, LANES), 1)


def rolled(value, shift):
    shift %= LANES
    return pltpu.roll(value, shift, 1) if shift else value


def depth_kernel(flags, x_ref, t1, t2, t3, from_lo, from_hi, t1_out, t2_out, t3_out, lo_out, hi_out):
    lane = lanes()
    low = jnp.where(flags[4] > 0, from_lo[...].astype(F32), 0.0)
    high = jnp.where(flags[5] > 0, from_hi[...].astype(F32), 0.0)

    def joined(own, mask_lo, shift_lo, mask_hi, shift_hi):
        value = own.astype(F32)
        value = jnp.where(mask_lo, rolled(low, shift_lo), value)
        return jnp.where(mask_hi, rolled(high, shift_hi), value)

    extra = []
    for x in range(2):
        for y in range(2):
            tile = 2 * x + y
            value = joined(
                t2[x, y], lane < 2, 32 - 2 * tile, (lane >= 34) & (lane < 36), 34 - 96 - 2 * tile
            )
            t2_out[x, y] = value.astype(BF16)
            extra.append(rolled(value, 72))
    value = joined(t3[...], lane < 2, 24, (lane >= 18) & (lane < 20), 18 - 104)
    t3_out[...] = value.astype(BF16)
    extra.append(rolled(value, 72))
    free = (lane >= 72) & (lane < 108)
    mask_lo = (lane >= 124) | (lane < 2)
    mask_hi = (lane >= 66) & (lane < 72)
    for x in range(4):
        for y in range(4):
            tile = 4 * x + y
            value = joined(t1[x, y], mask_lo, 124 - 6 * tile, mask_hi, 66 - 6 * tile)
            t1_out[x, y] = value.astype(BF16)
            k = tile % 8
            if k < 5:
                value = jnp.where(free, extra[k], value)
            (lo_out if x < 2 else hi_out)[8 + k] = value.astype(BF16)
    lo_out[0:8] = x_ref[0]
    hi_out[0:8] = x_ref[7]


def kept(flag, value):
    return jnp.where(flag > 0, value, jnp.zeros_like(value))


def width_kernel(flags, x_ref, t1, t2, t3, xr_lo, xr_hi, xr_lo2, xr_hi2, lo_out, hi_out, two_out):
    has_lo, has_hi, has_lo2, has_hi2 = flags[0], flags[1], flags[6], flags[7]
    lane = lanes()
    free = (lane >= 72) & (lane < 124)
    row = [
        rolled(kept(has_lo2, xr_lo2[...]).astype(F32), 0),
        rolled(kept(has_lo, xr_lo[12]).astype(F32), -72),
        t3[...].astype(F32),
        rolled(kept(has_hi, xr_hi[12]).astype(F32), -72),
        rolled(kept(has_hi2, xr_hi2[...]).astype(F32), 0),
    ]
    two = row[0]
    for i in range(1, 5):
        two = jnp.where(lane < 20 * i, two, rolled(row[i], 20 * i))
    two_out[...] = two.astype(BF16)
    coarse = [rolled(two, 72), rolled(two, 72 - 40), rolled(two, 72 - 80)]

    for out, fine_y, half_y in ((lo_out, 0, 0), (hi_out, 7, 2)):
        out[0] = kept(has_lo, xr_lo[fine_y])
        out[9] = kept(has_hi, xr_hi[fine_y])
        for x in range(8):
            out[1 + x] = x_ref[x, fine_y]
        for i in range(8):
            for k in range(2):
                y = half_y + k
                if i < 2:
                    value = kept(has_lo, xr_lo[8 + 4 * i + y])
                elif i < 6:
                    value = t1[i - 2, y]
                else:
                    value = kept(has_hi, xr_hi[8 + 4 * (i - 6) + y])
                if i < 2:
                    extra = kept(has_lo, xr_lo[8 + 2 * i + k]).astype(F32)
                elif i < 4:
                    extra = rolled(t2[i - 2, k].astype(F32), 72)
                elif i < 6:
                    extra = kept(has_hi, xr_hi[8 + 2 * (i - 4) + k]).astype(F32)
                else:
                    spot = 2 * (i - 6) + k
                    extra = coarse[spot] if spot < 3 else None
                if extra is not None:
                    value = jnp.where(free, extra, value.astype(F32)).astype(BF16)
                out[10 + 2 * i + k] = value


def weighted(weight, value):
    return lax.dot_general(weight, value, (((0,), (0,)), ((), ())), preferred_element_type=F32)


def spread(ref, i, j, value, base=0, lo=None, hi=None):
    lane = lanes()
    wide = value.astype(F32)
    before, after = rolled(wide, base + 1), rolled(wide, base - 1)
    if lo is not None:
        before = jnp.where(lane == 0, lo, before)
        after = jnp.where(lane == LANES - 1, hi, after)
    ref[i, j, 0:32] = before.astype(BF16)
    ref[i, j, 32:64] = rolled(wide, base).astype(BF16) if base else value
    ref[i, j, 64:96] = after.astype(BF16)


def block(w, dz):
    return jnp.concatenate([w[96 * k + 32 * dz : 96 * k + 32 * dz + 32] for k in range(9)], axis=0)


def weights_kernel(w0, w1, w2, w3, mix, f_out, a1_out, a2_out, a3_out):
    row = lax.broadcasted_iota(jnp.int32, (32, 96), 0)
    column = lax.broadcasted_iota(jnp.int32, (32, 96), 1)
    spots = [jnp.where(column == row + 32 * dz, 1.0, 0.0).astype(BF16) for dz in range(3)]

    def placed(dz, value):
        return lax.dot_general(spots[dz], value, (((0,), (1,)), ((), ())), preferred_element_type=F32)

    for w, out in ((w0, f_out), (w1, a1_out), (w2, a2_out), (w3, a3_out)):
        total = placed(0, block(w, 0)) + placed(1, block(w, 1)) + placed(2, block(w, 2))
        out[:, 0:288] = total.astype(BF16)
    mixed = lax.dot_general(spots[1], mix[...], (((0,), (0,)), ((), ())), preferred_element_type=F32)
    f_out[:, 288:320] = mixed.astype(BF16)


def around(ref, x, ys):
    return jnp.concatenate(
        [jnp.concatenate([ref[x + d, y : y + 3].reshape(96, LANES) for y in ys], axis=1) for d in range(3)],
        axis=0,
    )


def shifted(value, n, lo=None, hi=None):
    part = value[:, LANES * n : LANES * (n + 1)]
    before, after = rolled(part[0:32], 1), rolled(part[64:96], -1)
    if lo is not None:
        lane = lanes()
        before = jnp.where(lane == 0, lo, before)
        after = jnp.where(lane == LANES - 1, hi, after)
    return part[32:64] + before + after


def fine_kernel(x_ref, t1, w0, wf, acc_out, f0):
    lane = lanes()
    zero = jnp.zeros((32, LANES), BF16)
    for i in range(10):
        f0[i, 0] = zero
        f0[i, 9] = zero
        f0[0, i] = zero
        f0[9, i] = zero
    f0[1:9, 1:9] = x_ref[...]
    low = jnp.zeros((32, LANES), F32)
    high = jnp.zeros((32, LANES), F32)
    for i in range(4):
        for j in range(4):
            value = t1[i, j].astype(F32)
            for sx in range(2):
                spot = 12 * (2 * i + sx + 1) + 2 * j + 1
                here = (lane >= spot) & (lane < spot + 2)
                low = jnp.where(here, rolled(value, spot - 124 - 2 * sx), low)
                high = jnp.where(here, rolled(value, spot - 68 - 2 * sx), high)

    def columns(value, dz):
        near = [rolled(value, -12 * dx - dy).astype(BF16) for dx in (-1, 0, 1) for dy in (-1, 0, 1)]
        return weighted(block(w0, dz), jnp.concatenate(near, axis=0))

    low, high = columns(low, 0), columns(high, 2)
    for x in range(8):
        for y in range(0, 8, GROUP):
            ys = range(y, y + GROUP)
            middle = jnp.concatenate([x_ref[x, k] for k in ys], axis=1)
            value = dot(wf[...], jnp.concatenate([around(f0, x, ys), middle], axis=0))
            for n, k in enumerate(ys):
                spot = 12 * (x + 1) + k + 1
                acc_out[x, k] = shifted(value, n, rolled(low, -spot), rolled(high, 127 - spot))


def own_rows_kernel(
    flags, t1, t2, t3, xr_lo, xr_hi, xr_lo2, xr_hi2, w0, wf1, wf2, wf3,
    edge_out, a1_out, a2_out, a3_out, ex, f1, f2, f3,
):
    x_lo, x_hi, x_lo2, x_hi2 = flags[0], flags[1], flags[6], flags[7]
    zero = jnp.zeros((32, LANES), BF16)
    for ref, size in ((f1, 6), (f2, 4), (f3, 3)):
        for i in range(size + 2):
            for j in (0, 1, size, size + 1):
                ref[i, j] = zero
    for side in range(2):
        for j in (0, 9):
            ex[side, j] = jnp.zeros((96, LANES), BF16)
    for k in range(8):
        s = k % 2
        column = kept(x_lo, xr_lo[8 + 4 + k // 2]).astype(F32)
        spread(ex, 0, 1 + k, kept(x_lo, xr_lo[k]), 0, rolled(column, 2 - s), rolled(column, 57 - s))
        column = kept(x_hi, xr_hi[8 + k // 2]).astype(F32)
        spread(ex, 1, 1 + k, kept(x_hi, xr_hi[k]), 0, rolled(column, 4 - s), rolled(column, 59 - s))

    def back(value):
        return rolled(value.astype(F32), -72).astype(BF16)

    for k in range(4):
        for i in range(2):
            f1[i, 2 + k] = kept(x_lo, xr_lo[8 + 4 * i + k])
            f1[6 + i, 2 + k] = kept(x_hi, xr_hi[8 + 4 * i + k])
        for i in range(4):
            f1[2 + i, 2 + k] = t1[i, k]
    for i in range(2):
        for k in range(2):
            f2[i, 2 + k] = back(kept(x_lo, xr_lo[8 + 2 * i + k]))
            f2[2 + i, 2 + k] = t2[i, k]
            f2[4 + i, 2 + k] = back(kept(x_hi, xr_hi[8 + 2 * i + k]))
    f3[0, 2] = kept(x_lo2, xr_lo2[...])
    f3[1, 2] = back(kept(x_lo, xr_lo[12]))
    f3[2, 2] = t3[...]
    f3[3, 2] = back(kept(x_hi, xr_hi[12]))
    f3[4, 2] = kept(x_hi2, xr_hi2[...])

    for side, dx in ((0, 0), (1, 2)):
        weight = w0[288 * dx : 288 * dx + 288]
        for y in range(0, 8, 2):
            value = jnp.concatenate(
                [ex[side, y : y + 3].reshape(288, LANES), ex[side, y + 1 : y + 4].reshape(288, LANES)], axis=1
            )
            value = weighted(weight, value)
            edge_out[side, y] = value[:, :LANES]
            edge_out[side, y + 1] = value[:, LANES:]
    for ref, w, out, size in ((f3, wf3, a3_out, 3), (f2, wf2, a2_out, 4), (f1, wf1, a1_out, 6)):
        for i in range(size):
            value = dot(w[...], around(ref, i, range(size)))
            for j in range(size):
                out[i, j] = shifted(value, j)


def final_kernel(
    flags, acc, edge_x, a1, a2, a3, yr_lo, yr_hi, yr_two,
    w0, wf1, wf2, wf3, up, up0, out_hbm, ey, edge, f1, f2, f3, v3, v2, v1, q1, rows, out, sems,
):
    x_lo, x_hi, y_lo, y_hi, z_lo, z_hi = (flags[i] for i in range(6))
    y_lo2, y_hi2 = flags[8], flags[9]
    lane = lanes()

    zero = jnp.zeros((32, LANES), BF16)
    for ref, size in ((f1, 6), (f2, 4), (f3, 3)):
        for i in range(size + 2):
            for j in range(2, size):
                ref[i, j] = zero

    def back(flag, value, shift):
        return rolled(kept(flag, value).astype(F32), -shift).astype(BF16)

    for i in range(5):
        f3[i, 0] = back(y_lo2, yr_two[...], 20 * i)
        f3[i, 1] = back(y_lo, yr_lo[22 + i // 2], 72 + 20 * (i % 2))
        f3[i, 3] = back(y_hi, yr_hi[22 + i // 2], 72 + 20 * (i % 2))
        f3[i, 4] = back(y_hi2, yr_two[...], 20 * i)
    for i in range(6):
        for k in range(2):
            f2[i, k] = back(y_lo, yr_lo[10 + 2 * i + k], 72)
            f2[i, 4 + k] = back(y_hi, yr_hi[10 + 2 * i + k], 72)
    for i in range(8):
        for k in range(2):
            f1[i, k] = kept(y_lo, yr_lo[10 + 2 * i + k])
            f1[i, 6 + k] = kept(y_hi, yr_hi[10 + 2 * i + k])
    for i in range(10):
        sx = (i + 1) % 2
        coarse = (i + 1) // 2 + 1
        for side, ref, flag, row, s in ((0, yr_lo, y_lo, 1, 2 * sx + 1), (1, yr_hi, y_hi, 0, 2 * sx)):
            column = kept(flag, ref[10 + 2 * coarse + row]).astype(F32)
            spread(ey, side, i, kept(flag, ref[i]), 0, rolled(column, 4 - s), rolled(column, 59 - s))
    for side, dy in ((0, 0), (1, 2)):
        weight = jnp.concatenate([w0[96 * (3 * dx + dy) : 96 * (3 * dx + dy) + 96] for dx in range(3)], axis=0)
        for x in range(0, 8, 2):
            value = jnp.concatenate(
                [ey[side, x : x + 3].reshape(288, LANES), ey[side, x + 1 : x + 4].reshape(288, LANES)], axis=1
            )
            value = weighted(weight, value)
            edge[side, x] = value[:, :LANES]
            edge[side, x + 1] = value[:, LANES:]

    def along(before, centre, after):
        return [0.75 * centre + 0.25 * before, 0.75 * centre + 0.25 * after]

    def limits(count):
        inside = (lane >= 1) & (lane <= count + 2)
        inside &= (lane != 1) | (z_lo > 0)
        return inside & ((lane != count + 2) | (z_hi > 0))

    def cell_flag(position, last, lo, hi):
        return lo if position == 0 else hi if position == last else None

    def prolonged(ref, count):
        wide = dot(ref[...].reshape(count * count * 32, LANES), up[...]).reshape(count, count, 32, LANES)

        def refined(cells):
            out = []
            for k in range(2 * count - 2):
                cell = k - 1
                centre = cell // 2 + 1
                other = centre - 1 if cell % 2 == 0 else centre + 1
                out.append(0.75 * cells[centre] + 0.25 * cells[other])
            return out

        by_x = refined([wide[i] for i in range(count)])
        return [refined([row[j] for j in range(count)]) for row in by_x]

    def level(ref, w_ref, own, v_ref, size, cells, above):
        keep = limits(cells)
        touched = [j for j in range(size) if j < 2 or j >= size - 2]
        for x in range(size):
            value = dot(w_ref[...], around(ref, x, touched))
            for j in range(size):
                part = own[x, j]
                if j in touched:
                    part = part + shifted(value, touched.index(j))
                if above is not None:
                    part = part + above[x][j]
                good = keep
                for flag in (cell_flag(x, size - 1, x_lo, x_hi), cell_flag(j, size - 1, y_lo, y_hi)):
                    if flag is not None:
                        good = good & (flag > 0)
                v_ref[x, j] = jnp.where(good, part, 0.0).astype(BF16)

    level(f3, wf3, a3, v3, 3, 16, None)
    level(f2, wf2, a2, v2, 4, 32, prolonged(v3, 3))
    level(f1, wf1, a1, v1, 6, 64, prolonged(v2, 4))
    for i in range(6):
        q1[i] = dot(v1[i].reshape(6 * 32, LANES), up0[...]).reshape(6, 32, LANES)

    copies = []
    for x in range(8):
        c, part = x // 2, x % 2
        row = 0.75 * q1[c + 1] + 0.25 * q1[c + 2 * part]
        for y in range(0, 8, 2):
            centre = y // 2 + 1
            for n, extra in enumerate(along(row[centre - 1], row[centre], row[centre + 1])):
                total = acc[x, y + n] + extra
                if y + n == 0:
                    total = total + edge[0, x]
                if y + n == 7:
                    total = total + edge[1, x]
                if x == 0:
                    total = total + edge_x[0, y + n]
                if x == 7:
                    total = total + edge_x[1, y + n]
                rows[x, pl.ds(y + n, 32, stride=8), :] = jax.nn.gelu(total, approximate=True)
        out[x] = rows[x].reshape(32, 8, LANES).astype(BF16)
        copies.append(pltpu.make_async_copy(out.at[x], out_hbm.at[:, x], sems.at[x]))
        copies[-1].start()
    for copy in copies:
        copy.wait()


def turned(value, axis, step):
    count = lax.axis_size(axis)
    return lax.ppermute(value, axis, [(i, (i + step) % count) for i in range(count)])


def on_device(field, mixing, kernel_fine, kernel_half, kernel_quarter, kernel_eighth):
    gx, gy, gz = (lax.axis_index(a) for a in ("gx", "gy", "gz"))
    nx, ny, nz = (lax.axis_size(a) for a in ("gx", "gy", "gz"))
    slot = lax.iota(jnp.int32, 16)
    place = jnp.where((slot < 2) | (slot == 6) | (slot == 7), gx, jnp.where((slot == 4) | (slot == 5), gz, gy))
    side = slot & 1
    width = jnp.where(slot < 6, 1, 2)
    count = jnp.where((slot < 2) | (slot == 6) | (slot == 7), nx, jnp.where((slot == 4) | (slot == 5), nz, ny))
    flags = jnp.where(side == 0, place >= width, place < count - width).astype(jnp.int32)
    up, up0 = (jnp.asarray(m) for m in tables())
    tile = (32, LANES)

    (table,) = call(restrictions, [(512, 640)], [], scalars=0, flops=1 << 26)
    x_own, t1, t2, t3, msg = call(
        restrict_kernel,
        [(8, 8) + tile, (4, 4) + tile, (2, 2) + tile, tile, (2,) + tile],
        [field, table],
        [pltpu.VMEM((2048, LANES), F32)],
        0,
    )
    flat = [k.reshape(864, 32) for k in (kernel_fine, kernel_half, kernel_quarter, kernel_eighth)]
    mixing, *flat, t3 = lax.optimization_barrier((mixing, *flat, t3))
    wf = call(weights_kernel, [(96, 320)] + [(96, 288)] * 3, [*flat, mixing], scalars=0, flops=1 << 28)
    from_hi = turned(msg[0], "gz", -1)
    from_lo = turned(msg[1], "gz", 1)
    from_lo, *wf = lax.optimization_barrier((from_lo, *wf))
    t1, t2, t3, x_msg_lo, x_msg_hi = call(
        depth_kernel,
        [(4, 4) + tile, (2, 2) + tile, tile, (16,) + tile, (16,) + tile],
        [flags, x_own, t1, t2, t3, from_lo, from_hi],
    )
    xr_hi = turned(x_msg_lo, "gx", -1)
    xr_lo = turned(x_msg_hi, "gx", 1)
    xr_hi2 = turned(t3, "gx", -2)
    xr_lo2 = turned(t3, "gx", 2)
    (acc,) = call(
        fine_kernel,
        [(8, 8) + tile],
        [x_own, t1, flat[0], wf[0]],
        [pltpu.VMEM((10, 10) + tile, BF16)],
        0,
        kind=F32,
        flops=1 << 30,
    )
    xr_lo, acc = lax.optimization_barrier((xr_lo, acc))
    y_msg_lo, y_msg_hi, two = call(
        width_kernel,
        [(26,) + tile, (26,) + tile, tile],
        [flags, x_own, t1, t2, t3, xr_lo, xr_hi, xr_lo2, xr_hi2],
    )
    yr_hi = turned(y_msg_lo, "gy", -1)
    yr_lo = turned(y_msg_hi, "gy", 1)
    assert ny == 4
    yr_two = turned(two, "gy", 2)
    edge_x, a1, a2, a3 = call(
        own_rows_kernel,
        [(2, 8) + tile, (6, 6) + tile, (4, 4) + tile, (3, 3) + tile],
        [flags, t1, t2, t3, xr_lo, xr_hi, xr_lo2, xr_hi2, flat[0], *wf[1:]],
        [
            pltpu.VMEM((2, 10, 96, LANES), BF16),
            pltpu.VMEM((8, 8) + tile, BF16),
            pltpu.VMEM((6, 6) + tile, BF16),
            pltpu.VMEM((5, 5) + tile, BF16),
        ],
        kind=F32,
        flops=1 << 30,
    )
    (out,) = call(
        final_kernel,
        [(32, 8, 8, LANES)],
        [flags, acc, edge_x, a1, a2, a3, yr_lo, yr_hi, yr_two, flat[0], *wf[1:], up, up0],
        [
            pltpu.VMEM((2, 10, 96, LANES), BF16),
            pltpu.VMEM((2, 8) + tile, F32),
            pltpu.VMEM((8, 8) + tile, BF16),
            pltpu.VMEM((6, 6) + tile, BF16),
            pltpu.VMEM((5, 5) + tile, BF16),
            pltpu.VMEM((3, 3) + tile, BF16),
            pltpu.VMEM((4, 4) + tile, BF16),
            pltpu.VMEM((6, 6) + tile, BF16),
            pltpu.VMEM((6, 6) + tile, F32),
            pltpu.VMEM((8, 256, LANES), F32),
            pltpu.VMEM((8, 32, 8, LANES), BF16),
            pltpu.SemaphoreType.DMA((8,)),
        ],
        out_space=pl.ANY,
    )
    return out


def solution(mesh):
    placed = (P(None, "gx", "gy", "gz"), P(), P(), P(), P(), P())

    return jax.shard_map(on_device, mesh=mesh, in_specs=placed, out_specs=P(None, "gx", "gy", "gz"), check_vma=False)
```

```python
import jax
import jax.numpy as jnp
import numpy as np
from jax import lax
from jax.experimental import pallas as pl
from jax.experimental.pallas import tpu as pltpu
from jax.sharding import PartitionSpec as P


INTERPRET = False
F32, BF16 = jnp.float32, jnp.bfloat16
LANES = 128
GROUP = 4


def tables():
    up = np.zeros((128, 128), np.float32)
    up0 = np.zeros((128, 128), np.float32)
    for out in range(128):
        step = -1 if out % 2 == 0 else 1
        centre = out // 2 + 1
        if 0 <= centre + step:
            up[centre, out] += 0.75
            up[centre + step, out] += 0.25
        centre = out // 2 + 2
        up0[centre, out] += 0.75
        up0[centre + step, out] += 0.25
    return tuple(m.astype(BF16) for m in (up, up0))


def restrictions(table):
    row = lax.broadcasted_iota(jnp.int32, (512, LANES), 0)
    lane = lax.broadcasted_iota(jnp.int32, (1, LANES), 1)
    spot = row & 127
    eighth = jnp.float32(0.125)

    def put(k, *terms):
        value = jnp.zeros((512, LANES), F32)
        for mask, amount in terms:
            value = jnp.where(mask, amount, value)
        table[:, LANES * k : LANES * (k + 1)] = value.astype(BF16)

    def at(target, valid):
        return row == jnp.where(valid, target, -1)

    put(
        0,
        ((spot >> 1) + 2 == lane, eighth),
        (at((lane - 72) * 128, (lane >= 72) & (lane < 76)), 1.0),
        (at((lane - 76) * 128 + 127, (lane >= 76) & (lane < 80)), 1.0),
    )
    halves = ((spot - 2) >> 1) + 2 == lane
    sub = ((lane - 40) * 43) >> 8
    k = lane - 40 - 6 * sub
    low = at(sub * 128 + jnp.where(k < 2, 2 + k, 70 + k), (lane >= 40) & (lane < 64))
    sub = ((lane - 64) * 43) >> 8
    k = lane - 64 - 6 * sub
    high = at(sub * 128 + jnp.where(k < 4, 76 + k, 60 + k), (lane >= 64) & (lane < 88))
    put(1, (halves & (spot < 66) & (spot >= 2), eighth), (low, 1.0), (high, 1.0))
    put(2, (halves & (spot < 34) & (spot >= 2), eighth))
    tile = (lane * 43) >> 8
    k = lane - 6 * tile
    quad = (tile >> 3) * 2 + ((tile & 3) >> 1)
    sub = ((tile >> 2) & 1) * 2 + (tile & 1)
    last = (lane - 104) * 2
    for n, start, own, own3 in ((3, 40, 2, 2), (4, 64, 32, 30)):
        target = jnp.where(lane < 96, quad * 128 + start + 6 * sub + k, ((lane - 96) >> 1) * 128 + own + (lane & 1))
        tail = ((spot - own3) & ~1) == jnp.where((lane >= 104) & (lane < 106), last, -1000)
        put(n, (at(target, lane < 104), 1.0), (tail, eighth))


def dot(a, b):
    return jnp.dot(a, b, preferred_element_type=F32)


def call(kernel, outs, args, scratch=(), kind=BF16, flops=1 << 20, out_space=pltpu.VMEM):
    specs = [pl.BlockSpec(memory_space=pltpu.VMEM)] * len(args)
    return pl.pallas_call(
        kernel,
        out_shape=[jax.ShapeDtypeStruct(shape, kind) for shape in outs],
        in_specs=specs,
        out_specs=[pl.BlockSpec(memory_space=out_space)] * len(outs),
        scratch_shapes=list(scratch),
        compiler_params=pltpu.CompilerParams(vmem_limit_bytes=48 * 1024 * 1024),
        cost_estimate=pl.CostEstimate(flops=flops, transcendentals=0, bytes_accessed=1 << 20),
        interpret=INTERPRET,
    )(*args)


def restrict_kernel(field, table, x_out, t1_out, t2_out, t3_out, msg_out, rows):
    rows[...] = field[...].astype(F32).reshape(2048, LANES)
    for x in range(8):
        for y in range(8):
            x_out[x, y] = rows[pl.ds(x * 8 + y, 32, stride=64), :].astype(BF16)

    def four(ref, x, y):
        return jnp.concatenate(
            [ref[2 * x, 2 * y], ref[2 * x, 2 * y + 1], ref[2 * x + 1, 2 * y], ref[2 * x + 1, 2 * y + 1]],
            axis=1,
        )

    for x in range(4):
        left = jnp.concatenate([four(x_out, x, y) for y in range(4)], axis=0)
        t1_out[x] = dot(left, table[:, 0:128]).astype(BF16).reshape(4, 32, LANES)
    left = jnp.concatenate([four(t1_out, x, y) for x in range(2) for y in range(2)], axis=0)
    t2_out[...] = dot(left, table[:, 128:256]).astype(BF16).reshape(2, 2, 32, LANES)
    t3 = dot(four(t2_out, 0, 0), table[:, 256:640]).astype(BF16)
    t3_out[...] = t3[:, :128]
    msg_out[0] = t3[:, 128:256]
    msg_out[1] = t3[:, 256:]


def lanes():
    return lax.broadcasted_iota(jnp.int32, (32, LANES), 1)


def rolled(value, shift):
    shift %= LANES
    return pltpu.roll(value, shift, 1) if shift else value


def depth_kernel(flags, x_ref, t1, t2, t3, from_lo, from_hi, t1_out, t2_out, t3_out, lo_out, hi_out):
    lane = lanes()
    low = from_lo[...].astype(F32) * flags[4:5]
    high = from_hi[...].astype(F32) * flags[5:6]

    def joined(own, mask_lo, shift_lo, mask_hi, shift_hi):
        value = own.astype(F32)
        value = jnp.where(mask_lo, rolled(low, shift_lo), value)
        return jnp.where(mask_hi, rolled(high, shift_hi), value)

    extra = []
    for x in range(2):
        for y in range(2):
            tile = 2 * x + y
            value = joined(
                t2[x, y], lane < 2, 32 - 2 * tile, (lane >= 34) & (lane < 36), 34 - 96 - 2 * tile
            )
            t2_out[x, y] = value.astype(BF16)
            extra.append(rolled(value, 72))
    value = joined(t3[...], lane < 2, 24, (lane >= 18) & (lane < 20), 18 - 104)
    t3_out[...] = value.astype(BF16)
    extra.append(rolled(value, 72))
    free = (lane >= 72) & (lane < 108)
    mask_lo = (lane >= 124) | (lane < 2)
    mask_hi = (lane >= 66) & (lane < 72)
    for x in range(4):
        for y in range(4):
            tile = 4 * x + y
            value = joined(t1[x, y], mask_lo, 124 - 6 * tile, mask_hi, 66 - 6 * tile)
            t1_out[x, y] = value.astype(BF16)
            k = tile % 8
            if k < 5:
                value = jnp.where(free, extra[k], value)
            (lo_out if x < 2 else hi_out)[8 + k] = value.astype(BF16)
    lo_out[0:8] = x_ref[0]
    hi_out[0:8] = x_ref[7]


def kept(flag, value):
    return value * jnp.broadcast_to(flag, value.shape).astype(BF16)


def width_kernel(flags, x_ref, t1, t2, t3, xr_lo, xr_hi, xr_lo2, xr_hi2, lo_out, hi_out, two_out):
    has_lo, has_hi, has_lo2, has_hi2 = flags[0:1], flags[1:2], flags[6:7], flags[7:8]
    lane = lanes()
    free = (lane >= 72) & (lane < 124)
    row = [
        rolled(kept(has_lo2, xr_lo2[...]).astype(F32), 0),
        rolled(kept(has_lo, xr_lo[12]).astype(F32), -72),
        t3[...].astype(F32),
        rolled(kept(has_hi, xr_hi[12]).astype(F32), -72),
        rolled(kept(has_hi2, xr_hi2[...]).astype(F32), 0),
    ]
    two = row[0]
    for i in range(1, 5):
        two = jnp.where(lane < 20 * i, two, rolled(row[i], 20 * i))
    two_out[...] = two.astype(BF16)
    coarse = [rolled(two, 72), rolled(two, 72 - 40), rolled(two, 72 - 80)]

    for out, fine_y, half_y in ((lo_out, 0, 0), (hi_out, 7, 2)):
        out[0] = kept(has_lo, xr_lo[fine_y])
        out[9] = kept(has_hi, xr_hi[fine_y])
        for x in range(8):
            out[1 + x] = x_ref[x, fine_y]
        for i in range(8):
            for k in range(2):
                y = half_y + k
                if i < 2:
                    value = kept(has_lo, xr_lo[8 + 4 * i + y])
                elif i < 6:
                    value = t1[i - 2, y]
                else:
                    value = kept(has_hi, xr_hi[8 + 4 * (i - 6) + y])
                if i < 2:
                    extra = kept(has_lo, xr_lo[8 + 2 * i + k]).astype(F32)
                elif i < 4:
                    extra = rolled(t2[i - 2, k].astype(F32), 72)
                elif i < 6:
                    extra = kept(has_hi, xr_hi[8 + 2 * (i - 4) + k]).astype(F32)
                else:
                    spot = 2 * (i - 6) + k
                    extra = coarse[spot] if spot < 3 else None
                if extra is not None:
                    value = jnp.where(free, extra, value.astype(F32)).astype(BF16)
                out[10 + 2 * i + k] = value


def weighted(weight, value):
    return lax.dot_general(weight, value, (((0,), (0,)), ((), ())), preferred_element_type=F32)


def spread(ref, i, j, value, base=0, lo=None, hi=None):
    lane = lanes()
    wide = value.astype(F32)
    before, after = rolled(wide, base + 1), rolled(wide, base - 1)
    if lo is not None:
        before = jnp.where(lane == 0, lo, before)
        after = jnp.where(lane == LANES - 1, hi, after)
    ref[i, j, 0:32] = before.astype(BF16)
    ref[i, j, 32:64] = rolled(wide, base).astype(BF16) if base else value
    ref[i, j, 64:96] = after.astype(BF16)


def block(w, dz):
    return jnp.concatenate([w[96 * k + 32 * dz : 96 * k + 32 * dz + 32] for k in range(9)], axis=0)


def weights_kernel(w0, w1, w2, w3, mix, f_out, a1_out, a2_out, a3_out):
    row = lax.broadcasted_iota(jnp.int32, (32, 96), 0)
    column = lax.broadcasted_iota(jnp.int32, (32, 96), 1)
    spots = [jnp.where(column == row + 32 * dz, 1.0, 0.0).astype(BF16) for dz in range(3)]

    def placed(dz, value):
        return lax.dot_general(spots[dz], value, (((0,), (1,)), ((), ())), preferred_element_type=F32)

    for w, out in ((w0, f_out), (w1, a1_out), (w2, a2_out), (w3, a3_out)):
        total = placed(0, block(w, 0)) + placed(1, block(w, 1)) + placed(2, block(w, 2))
        out[:, 0:288] = total.astype(BF16)
    mixed = lax.dot_general(spots[1], mix[...], (((0,), (0,)), ((), ())), preferred_element_type=F32)
    f_out[:, 288:320] = mixed.astype(BF16)


def around(ref, x, ys):
    return jnp.concatenate(
        [jnp.concatenate([ref[x + d, y : y + 3].reshape(96, LANES) for y in ys], axis=1) for d in range(3)],
        axis=0,
    )


def shifted(value, n, lo=None, hi=None):
    part = value[:, LANES * n : LANES * (n + 1)]
    before, after = rolled(part[0:32], 1), rolled(part[64:96], -1)
    if lo is not None:
        lane = lanes()
        before = jnp.where(lane == 0, lo, before)
        after = jnp.where(lane == LANES - 1, hi, after)
    return part[32:64] + before + after


def fine_kernel(x_ref, t1, w0, wf, acc_out, f0):
    lane = lanes()
    zero = jnp.zeros((32, LANES), BF16)
    for i in range(10):
        f0[i, 0] = zero
        f0[i, 9] = zero
        f0[0, i] = zero
        f0[9, i] = zero
    f0[1:9, 1:9] = x_ref[...]
    low = jnp.zeros((32, LANES), F32)
    high = jnp.zeros((32, LANES), F32)
    for i in range(4):
        for j in range(4):
            value = t1[i, j].astype(F32)
            for sx in range(2):
                spot = 12 * (2 * i + sx + 1) + 2 * j + 1
                here = (lane >= spot) & (lane < spot + 2)
                low = jnp.where(here, rolled(value, spot - 124 - 2 * sx), low)
                high = jnp.where(here, rolled(value, spot - 68 - 2 * sx), high)

    def columns(value, dz):
        near = [rolled(value, -12 * dx - dy).astype(BF16) for dx in (-1, 0, 1) for dy in (-1, 0, 1)]
        return weighted(block(w0, dz), jnp.concatenate(near, axis=0))

    low, high = columns(low, 0), columns(high, 2)
    for x in range(8):
        for y in range(0, 8, GROUP):
            ys = range(y, y + GROUP)
            middle = jnp.concatenate([x_ref[x, k] for k in ys], axis=1)
            value = dot(wf[...], jnp.concatenate([around(f0, x, ys), middle], axis=0))
            for n, k in enumerate(ys):
                spot = 12 * (x + 1) + k + 1
                acc_out[x, k] = shifted(value, n, rolled(low, -spot), rolled(high, 127 - spot))


def own_rows_kernel(
    flags, t1, t2, t3, xr_lo, xr_hi, xr_lo2, xr_hi2, w0, wf1, wf2, wf3,
    edge_out, a1_out, a2_out, a3_out, ex, f1, f2, f3,
):
    x_lo, x_hi, x_lo2, x_hi2 = flags[0:1], flags[1:2], flags[6:7], flags[7:8]
    zero = jnp.zeros((32, LANES), BF16)
    for ref, size in ((f1, 6), (f2, 4), (f3, 3)):
        for i in range(size + 2):
            for j in (0, 1, size, size + 1):
                ref[i, j] = zero
    for side in range(2):
        for j in (0, 9):
            ex[side, j] = jnp.zeros((96, LANES), BF16)
    for k in range(8):
        s = k % 2
        column = kept(x_lo, xr_lo[8 + 4 + k // 2]).astype(F32)
        spread(ex, 0, 1 + k, kept(x_lo, xr_lo[k]), 0, rolled(column, 2 - s), rolled(column, 57 - s))
        column = kept(x_hi, xr_hi[8 + k // 2]).astype(F32)
        spread(ex, 1, 1 + k, kept(x_hi, xr_hi[k]), 0, rolled(column, 4 - s), rolled(column, 59 - s))

    def back(value):
        return rolled(value.astype(F32), -72).astype(BF16)

    for k in range(4):
        for i in range(2):
            f1[i, 2 + k] = kept(x_lo, xr_lo[8 + 4 * i + k])
            f1[6 + i, 2 + k] = kept(x_hi, xr_hi[8 + 4 * i + k])
        for i in range(4):
            f1[2 + i, 2 + k] = t1[i, k]
    for i in range(2):
        for k in range(2):
            f2[i, 2 + k] = back(kept(x_lo, xr_lo[8 + 2 * i + k]))
            f2[2 + i, 2 + k] = t2[i, k]
            f2[4 + i, 2 + k] = back(kept(x_hi, xr_hi[8 + 2 * i + k]))
    f3[0, 2] = kept(x_lo2, xr_lo2[...])
    f3[1, 2] = back(kept(x_lo, xr_lo[12]))
    f3[2, 2] = t3[...]
    f3[3, 2] = back(kept(x_hi, xr_hi[12]))
    f3[4, 2] = kept(x_hi2, xr_hi2[...])

    for side, dx in ((0, 0), (1, 2)):
        weight = w0[288 * dx : 288 * dx + 288]
        for y in range(0, 8, 2):
            value = jnp.concatenate(
                [ex[side, y : y + 3].reshape(288, LANES), ex[side, y + 1 : y + 4].reshape(288, LANES)], axis=1
            )
            value = weighted(weight, value)
            edge_out[side, y] = value[:, :LANES]
            edge_out[side, y + 1] = value[:, LANES:]
    for ref, w, out, size in ((f3, wf3, a3_out, 3), (f2, wf2, a2_out, 4), (f1, wf1, a1_out, 6)):
        for i in range(size):
            value = dot(w[...], around(ref, i, range(size)))
            for j in range(size):
                out[i, j] = shifted(value, j)


def final_kernel(
    flags, acc, edge_x, a1, a2, a3, yr_lo, yr_hi, yr_two,
    w0, wf1, wf2, wf3, up, up0, out_hbm, ey, edge, f1, f2, f3, v3, v2, v1, q1, rows, out, sems,
):
    x_lo, x_hi, y_lo, y_hi, z_lo, z_hi = (flags[i : i + 1] for i in range(6))
    y_lo2, y_hi2 = flags[8:9], flags[9:10]
    lane = lanes()

    zero = jnp.zeros((32, LANES), BF16)
    for ref, size in ((f1, 6), (f2, 4), (f3, 3)):
        for i in range(size + 2):
            for j in range(2, size):
                ref[i, j] = zero

    def back(flag, value, shift):
        return rolled(kept(flag, value).astype(F32), -shift).astype(BF16)

    for i in range(5):
        f3[i, 0] = back(y_lo2, yr_two[...], 20 * i)
        f3[i, 1] = back(y_lo, yr_lo[22 + i // 2], 72 + 20 * (i % 2))
        f3[i, 3] = back(y_hi, yr_hi[22 + i // 2], 72 + 20 * (i % 2))
        f3[i, 4] = back(y_hi2, yr_two[...], 20 * i)
    for i in range(6):
        for k in range(2):
            f2[i, k] = back(y_lo, yr_lo[10 + 2 * i + k], 72)
            f2[i, 4 + k] = back(y_hi, yr_hi[10 + 2 * i + k], 72)
    for i in range(8):
        for k in range(2):
            f1[i, k] = kept(y_lo, yr_lo[10 + 2 * i + k])
            f1[i, 6 + k] = kept(y_hi, yr_hi[10 + 2 * i + k])
    for i in range(10):
        sx = (i + 1) % 2
        coarse = (i + 1) // 2 + 1
        for side, ref, flag, row, s in ((0, yr_lo, y_lo, 1, 2 * sx + 1), (1, yr_hi, y_hi, 0, 2 * sx)):
            column = kept(flag, ref[10 + 2 * coarse + row]).astype(F32)
            spread(ey, side, i, kept(flag, ref[i]), 0, rolled(column, 4 - s), rolled(column, 59 - s))
    for side, dy in ((0, 0), (1, 2)):
        weight = jnp.concatenate([w0[96 * (3 * dx + dy) : 96 * (3 * dx + dy) + 96] for dx in range(3)], axis=0)
        for x in range(0, 8, 2):
            value = jnp.concatenate(
                [ey[side, x : x + 3].reshape(288, LANES), ey[side, x + 1 : x + 4].reshape(288, LANES)], axis=1
            )
            value = weighted(weight, value)
            edge[side, x] = value[:, :LANES]
            edge[side, x + 1] = value[:, LANES:]

    def along(before, centre, after):
        return [0.75 * centre + 0.25 * before, 0.75 * centre + 0.25 * after]

    def limits(count):
        spot = lax.broadcasted_iota(jnp.int32, (1, LANES), 1)
        inside = jnp.where((spot >= 1) & (spot <= count + 2), 1.0, 0.0)
        return jnp.where(spot == 1, z_lo, jnp.where(spot == count + 2, z_hi, inside))

    def cell_flag(position, last, lo, hi):
        return lo if position == 0 else hi if position == last else None

    def prolonged(ref, count):
        wide = dot(ref[...].reshape(count * count * 32, LANES), up[...]).reshape(count, count, 32, LANES)

        def refined(cells):
            out = []
            for k in range(2 * count - 2):
                cell = k - 1
                centre = cell // 2 + 1
                other = centre - 1 if cell % 2 == 0 else centre + 1
                out.append(0.75 * cells[centre] + 0.25 * cells[other])
            return out

        by_x = refined([wide[i] for i in range(count)])
        return [refined([row[j] for j in range(count)]) for row in by_x]

    def level(ref, w_ref, own, v_ref, size, cells, above):
        keep = limits(cells)
        touched = [j for j in range(size) if j < 2 or j >= size - 2]
        for x in range(size):
            value = dot(w_ref[...], around(ref, x, touched))
            for j in range(size):
                part = own[x, j]
                if j in touched:
                    part = part + shifted(value, touched.index(j))
                if above is not None:
                    part = part + above[x][j]
                good = keep
                for flag in (cell_flag(x, size - 1, x_lo, x_hi), cell_flag(j, size - 1, y_lo, y_hi)):
                    if flag is not None:
                        good = good * flag
                v_ref[x, j] = (part * good).astype(BF16)

    level(f3, wf3, a3, v3, 3, 16, None)
    level(f2, wf2, a2, v2, 4, 32, prolonged(v3, 3))
    level(f1, wf1, a1, v1, 6, 64, prolonged(v2, 4))
    for i in range(6):
        q1[i] = dot(v1[i].reshape(6 * 32, LANES), up0[...]).reshape(6, 32, LANES)

    copies = []
    for x in range(8):
        c, part = x // 2, x % 2
        row = 0.75 * q1[c + 1] + 0.25 * q1[c + 2 * part]
        for y in range(0, 8, 2):
            centre = y // 2 + 1
            for n, extra in enumerate(along(row[centre - 1], row[centre], row[centre + 1])):
                total = acc[x, y + n] + extra
                if y + n == 0:
                    total = total + edge[0, x]
                if y + n == 7:
                    total = total + edge[1, x]
                if x == 0:
                    total = total + edge_x[0, y + n]
                if x == 7:
                    total = total + edge_x[1, y + n]
                rows[x, pl.ds(y + n, 32, stride=8), :] = jax.nn.gelu(total, approximate=True)
        out[x] = rows[x].reshape(32, 8, LANES).astype(BF16)
        copies.append(pltpu.make_async_copy(out.at[x], out_hbm.at[:, x], sems.at[x]))
        copies[-1].start()
    for copy in copies:
        copy.wait()


def turned(value, axis, step):
    count = lax.axis_size(axis)
    return lax.ppermute(value, axis, [(i, (i + step) % count) for i in range(count)])


def on_device(field, mixing, kernel_fine, kernel_half, kernel_quarter, kernel_eighth):
    gx, gy, gz = (lax.axis_index(a) for a in ("gx", "gy", "gz"))
    nx, ny, nz = (lax.axis_size(a) for a in ("gx", "gy", "gz"))
    slot = lax.broadcasted_iota(jnp.int32, (16, LANES), 0)
    place = jnp.where((slot < 2) | (slot == 6) | (slot == 7), gx, jnp.where((slot == 4) | (slot == 5), gz, gy))
    side = slot & 1
    width = jnp.where(slot < 6, 1, 2)
    count = jnp.where((slot < 2) | (slot == 6) | (slot == 7), nx, jnp.where((slot == 4) | (slot == 5), nz, ny))
    flags = jnp.where(side == 0, place >= width, place < count - width).astype(F32)
    up, up0 = (jnp.asarray(m) for m in tables())
    tile = (32, LANES)

    (table,) = call(restrictions, [(512, 640)], [], flops=1 << 26)
    x_own, t1, t2, t3, msg = call(
        restrict_kernel,
        [(8, 8) + tile, (4, 4) + tile, (2, 2) + tile, tile, (2,) + tile],
        [field, table],
        [pltpu.VMEM((2048, LANES), F32)],
    )
    flat = [k.reshape(864, 32) for k in (kernel_fine, kernel_half, kernel_quarter, kernel_eighth)]
    mixing, *flat, t3 = lax.optimization_barrier((mixing, *flat, t3))
    wf = call(weights_kernel, [(96, 320)] + [(96, 288)] * 3, [*flat, mixing], flops=1 << 28)
    from_hi = turned(msg[0], "gz", -1)
    from_lo = turned(msg[1], "gz", 1)
    from_lo, *wf = lax.optimization_barrier((from_lo, *wf))
    t1, t2, t3, x_msg_lo, x_msg_hi = call(
        depth_kernel,
        [(4, 4) + tile, (2, 2) + tile, tile, (16,) + tile, (16,) + tile],
        [flags, x_own, t1, t2, t3, from_lo, from_hi],
    )
    xr_hi = turned(x_msg_lo, "gx", -1)
    xr_lo = turned(x_msg_hi, "gx", 1)
    xr_hi2 = turned(t3, "gx", -2)
    xr_lo2 = turned(t3, "gx", 2)
    (acc,) = call(
        fine_kernel,
        [(8, 8) + tile],
        [x_own, t1, flat[0], wf[0]],
        [pltpu.VMEM((10, 10) + tile, BF16)],
        kind=F32,
        flops=1 << 30,
    )
    xr_lo, acc = lax.optimization_barrier((xr_lo, acc))
    y_msg_lo, y_msg_hi, two = call(
        width_kernel,
        [(26,) + tile, (26,) + tile, tile],
        [flags, x_own, t1, t2, t3, xr_lo, xr_hi, xr_lo2, xr_hi2],
    )
    yr_hi = turned(y_msg_lo, "gy", -1)
    yr_lo = turned(y_msg_hi, "gy", 1)
    assert ny == 4
    yr_two = turned(two, "gy", 2)
    edge_x, a1, a2, a3 = call(
        own_rows_kernel,
        [(2, 8) + tile, (6, 6) + tile, (4, 4) + tile, (3, 3) + tile],
        [flags, t1, t2, t3, xr_lo, xr_hi, xr_lo2, xr_hi2, flat[0], *wf[1:]],
        [
            pltpu.VMEM((2, 10, 96, LANES), BF16),
            pltpu.VMEM((8, 8) + tile, BF16),
            pltpu.VMEM((6, 6) + tile, BF16),
            pltpu.VMEM((5, 5) + tile, BF16),
        ],
        kind=F32,
        flops=1 << 30,
    )
    (out,) = call(
        final_kernel,
        [(32, 8, 8, LANES)],
        [flags, acc, edge_x, a1, a2, a3, yr_lo, yr_hi, yr_two, flat[0], *wf[1:], up, up0],
        [
            pltpu.VMEM((2, 10, 96, LANES), BF16),
            pltpu.VMEM((2, 8) + tile, F32),
            pltpu.VMEM((8, 8) + tile, BF16),
            pltpu.VMEM((6, 6) + tile, BF16),
            pltpu.VMEM((5, 5) + tile, BF16),
            pltpu.VMEM((3, 3) + tile, BF16),
            pltpu.VMEM((4, 4) + tile, BF16),
            pltpu.VMEM((6, 6) + tile, BF16),
            pltpu.VMEM((6, 6) + tile, F32),
            pltpu.VMEM((8, 256, LANES), F32),
            pltpu.VMEM((8, 32, 8, LANES), BF16),
            pltpu.SemaphoreType.DMA((8,)),
        ],
        out_space=pl.ANY,
    )
    return out


def solution(mesh):
    placed = (P(None, "gx", "gy", "gz"), P(), P(), P(), P(), P())

    return jax.shard_map(on_device, mesh=mesh, in_specs=placed, out_specs=P(None, "gx", "gy", "gz"), check_vma=False)
```

```python
import jax
import jax.numpy as jnp
import numpy as np
from jax import lax
from jax.experimental import pallas as pl
from jax.experimental.pallas import tpu as pltpu
from jax.sharding import PartitionSpec as P


INTERPRET = False
F32, BF16 = jnp.float32, jnp.bfloat16
LANES = 128
GROUP = 8


def tables():
    up = np.zeros((128, 128), np.float32)
    up0 = np.zeros((128, 128), np.float32)
    for out in range(128):
        step = -1 if out % 2 == 0 else 1
        centre = out // 2 + 1
        if 0 <= centre + step:
            up[centre, out] += 0.75
            up[centre + step, out] += 0.25
        centre = out // 2 + 2
        up0[centre, out] += 0.75
        up0[centre + step, out] += 0.25
    return tuple(m.astype(BF16) for m in (up, up0))


def restrictions(table):
    row = lax.broadcasted_iota(jnp.int32, (512, LANES), 0)
    lane = lax.broadcasted_iota(jnp.int32, (1, LANES), 1)
    spot = row & 127
    eighth = jnp.float32(0.125)

    def put(k, *terms):
        value = jnp.zeros((512, LANES), F32)
        for mask, amount in terms:
            value = jnp.where(mask, amount, value)
        table[:, LANES * k : LANES * (k + 1)] = value.astype(BF16)

    def at(target, valid):
        return row == jnp.where(valid, target, -1)

    put(
        0,
        ((spot >> 1) + 2 == lane, eighth),
        (at((lane - 72) * 128, (lane >= 72) & (lane < 76)), 1.0),
        (at((lane - 76) * 128 + 127, (lane >= 76) & (lane < 80)), 1.0),
    )
    halves = ((spot - 2) >> 1) + 2 == lane
    sub = ((lane - 40) * 43) >> 8
    k = lane - 40 - 6 * sub
    low = at(sub * 128 + jnp.where(k < 2, 2 + k, 70 + k), (lane >= 40) & (lane < 64))
    sub = ((lane - 64) * 43) >> 8
    k = lane - 64 - 6 * sub
    high = at(sub * 128 + jnp.where(k < 4, 76 + k, 60 + k), (lane >= 64) & (lane < 88))
    put(1, (halves & (spot < 66) & (spot >= 2), eighth), (low, 1.0), (high, 1.0))
    put(2, (halves & (spot < 34) & (spot >= 2), eighth))
    tile = (lane * 43) >> 8
    k = lane - 6 * tile
    quad = (tile >> 3) * 2 + ((tile & 3) >> 1)
    sub = ((tile >> 2) & 1) * 2 + (tile & 1)
    last = (lane - 104) * 2
    for n, start, own, own3 in ((3, 40, 2, 2), (4, 64, 32, 30)):
        target = jnp.where(lane < 96, quad * 128 + start + 6 * sub + k, ((lane - 96) >> 1) * 128 + own + (lane & 1))
        tail = ((spot - own3) & ~1) == jnp.where((lane >= 104) & (lane < 106), last, -1000)
        put(n, (at(target, lane < 104), 1.0), (tail, eighth))


def dot(a, b):
    return jnp.dot(a, b, preferred_element_type=F32)


def call(kernel, outs, args, scratch=(), kind=BF16, flops=1 << 20, out_space=pltpu.VMEM):
    specs = [pl.BlockSpec(memory_space=pltpu.VMEM)] * len(args)
    return pl.pallas_call(
        kernel,
        out_shape=[jax.ShapeDtypeStruct(shape, kind) for shape in outs],
        in_specs=specs,
        out_specs=[pl.BlockSpec(memory_space=out_space)] * len(outs),
        scratch_shapes=list(scratch),
        compiler_params=pltpu.CompilerParams(vmem_limit_bytes=48 * 1024 * 1024),
        cost_estimate=pl.CostEstimate(flops=flops, transcendentals=0, bytes_accessed=1 << 20),
        interpret=INTERPRET,
    )(*args)


def restrict_kernel(field, table, x_out, t1_out, t2_out, t3_out, msg_out, rows):
    rows[...] = field[...].astype(F32).reshape(2048, LANES)
    for x in range(8):
        for y in range(8):
            x_out[x, y] = rows[pl.ds(x * 8 + y, 32, stride=64), :].astype(BF16)

    def four(ref, x, y):
        return jnp.concatenate(
            [ref[2 * x, 2 * y], ref[2 * x, 2 * y + 1], ref[2 * x + 1, 2 * y], ref[2 * x + 1, 2 * y + 1]],
            axis=1,
        )

    for x in range(4):
        left = jnp.concatenate([four(x_out, x, y) for y in range(4)], axis=0)
        t1_out[x] = dot(left, table[:, 0:128]).astype(BF16).reshape(4, 32, LANES)
    left = jnp.concatenate([four(t1_out, x, y) for x in range(2) for y in range(2)], axis=0)
    t2_out[...] = dot(left, table[:, 128:256]).astype(BF16).reshape(2, 2, 32, LANES)
    t3 = dot(four(t2_out, 0, 0), table[:, 256:640]).astype(BF16)
    t3_out[...] = t3[:, :128]
    msg_out[0] = t3[:, 128:256]
    msg_out[1] = t3[:, 256:]


def lanes():
    return lax.broadcasted_iota(jnp.int32, (32, LANES), 1)


def rolled(value, shift):
    shift %= LANES
    return pltpu.roll(value, shift, 1) if shift else value


def depth_kernel(flags, x_ref, t1, t2, t3, from_lo, from_hi, t1_out, t2_out, t3_out, lo_out, hi_out, ylo_out, yhi_out):
    lane = lanes()
    low = from_lo[...].astype(F32) * flags[4:5]
    high = from_hi[...].astype(F32) * flags[5:6]

    def joined(own, mask_lo, shift_lo, mask_hi, shift_hi):
        value = own.astype(F32)
        value = jnp.where(mask_lo, rolled(low, shift_lo), value)
        return jnp.where(mask_hi, rolled(high, shift_hi), value)

    extra = []
    for x in range(2):
        for y in range(2):
            tile = 2 * x + y
            value = joined(
                t2[x, y], lane < 2, 32 - 2 * tile, (lane >= 34) & (lane < 36), 34 - 96 - 2 * tile
            )
            t2_out[x, y] = value.astype(BF16)
            extra.append(rolled(value, 72))
    value = joined(t3[...], lane < 2, 24, (lane >= 18) & (lane < 20), 18 - 104)
    t3_out[...] = value.astype(BF16)
    extra.append(rolled(value, 72))
    free = (lane >= 72) & (lane < 108)
    mask_lo = (lane >= 124) | (lane < 2)
    mask_hi = (lane >= 66) & (lane < 72)
    for x in range(4):
        for y in range(4):
            tile = 4 * x + y
            value = joined(t1[x, y], mask_lo, 124 - 6 * tile, mask_hi, 66 - 6 * tile)
            t1_out[x, y] = value.astype(BF16)
            k = tile % 8
            joint = jnp.where(free, extra[k], value) if k < 5 else value
            (lo_out if x < 2 else hi_out)[8 + k] = joint.astype(BF16)
            k = 2 * x + y % 2
            joint = jnp.where(free, extra[k], value) if k < 4 else value
            (ylo_out if y < 2 else yhi_out)[8 + k] = joint.astype(BF16)
    lo_out[0:8] = x_ref[0]
    hi_out[0:8] = x_ref[7]
    for x in range(8):
        ylo_out[x] = x_ref[x, 0]
        yhi_out[x] = x_ref[x, 7]


def kept(flag, value):
    return value * jnp.broadcast_to(flag, value.shape).astype(BF16)


def width_kernel(flags, t3, xr_lo, xr_hi, xr_lo2, xr_hi2, lo_out, hi_out, two_out):
    has_lo, has_hi, has_lo2, has_hi2 = flags[0:1], flags[1:2], flags[6:7], flags[7:8]
    lane = lanes()
    free = (lane >= 72) & (lane < 124)
    row = [
        kept(has_lo2, xr_lo2[...]).astype(F32),
        rolled(kept(has_lo, xr_lo[12]).astype(F32), -72),
        t3[...].astype(F32),
        rolled(kept(has_hi, xr_hi[12]).astype(F32), -72),
        kept(has_hi2, xr_hi2[...]).astype(F32),
    ]
    two = row[0]
    for i in range(1, 5):
        two = jnp.where(lane < 20 * i, two, rolled(row[i], 20 * i))
    two = two.astype(BF16)
    two_out[...] = two
    for out, fine_y, half_y in ((lo_out, 0, 0), (hi_out, 7, 2)):
        out[0] = kept(has_lo, xr_lo[fine_y])
        out[1] = kept(has_hi, xr_hi[fine_y])
        for i in range(4):
            flag, ref = (has_lo, xr_lo) if i < 2 else (has_hi, xr_hi)
            for k in range(2):
                value = ref[8 + 4 * (i % 2) + half_y + k].astype(F32)
                extra = ref[8 + 2 * (i % 2) + k].astype(F32)
                out[2 + 2 * i + k] = kept(flag, jnp.where(free, extra, value).astype(BF16))
        out[10] = two


def fine_row(near, far, i):
    return far[0] if i == 0 else far[1] if i == 9 else near[i - 1]


def half_tile(near, far, i, k):
    return near[4 + 2 * i + k] if 2 <= i < 6 else far[2 + 2 * (i % 4) + k if i < 2 else 2 + 2 * (i - 4) + k]


def quarter_tile(near, far, i, k):
    return near[4 + 2 * i + k] if 2 <= i < 4 else far[2 + 2 * i + k if i < 2 else 2 + 2 * (i - 2) + k]


def weighted(weight, value):
    return lax.dot_general(weight, value, (((0,), (0,)), ((), ())), preferred_element_type=F32)


def spread(ref, i, j, value, base=0, lo=None, hi=None):
    lane = lanes()
    wide = value.astype(F32)
    before, after = rolled(wide, base + 1), rolled(wide, base - 1)
    if lo is not None:
        before = jnp.where(lane == 0, lo, before)
        after = jnp.where(lane == LANES - 1, hi, after)
    ref[i, j, 0:32] = before.astype(BF16)
    ref[i, j, 32:64] = rolled(wide, base).astype(BF16) if base else value
    ref[i, j, 64:96] = after.astype(BF16)


def block(w, dz):
    return jnp.concatenate([w[96 * k + 32 * dz : 96 * k + 32 * dz + 32] for k in range(9)], axis=0)


def weights_kernel(w0, w1, w2, w3, mix, f_out, a1_out, a2_out, a3_out):
    row = lax.broadcasted_iota(jnp.int32, (32, 96), 0)
    column = lax.broadcasted_iota(jnp.int32, (32, 96), 1)
    spots = [jnp.where(column == row + 32 * dz, 1.0, 0.0).astype(BF16) for dz in range(3)]

    def placed(dz, value):
        return lax.dot_general(spots[dz], value, (((0,), (1,)), ((), ())), preferred_element_type=F32)

    for w, out in ((w0, f_out), (w1, a1_out), (w2, a2_out), (w3, a3_out)):
        total = placed(0, block(w, 0)) + placed(1, block(w, 1)) + placed(2, block(w, 2))
        out[:, 0:288] = total.astype(BF16)
    mixed = lax.dot_general(spots[1], mix[...], (((0,), (0,)), ((), ())), preferred_element_type=F32)
    f_out[:, 288:320] = mixed.astype(BF16)


def around(ref, x, ys):
    return jnp.concatenate(
        [jnp.concatenate([ref[x + d, y : y + 3].reshape(96, LANES) for y in ys], axis=1) for d in range(3)],
        axis=0,
    )


def shifted(value, n, lo=None, hi=None):
    part = value[:, LANES * n : LANES * (n + 1)]
    before, after = rolled(part[0:32], 1), rolled(part[64:96], -1)
    if lo is not None:
        lane = lanes()
        before = jnp.where(lane == 0, lo, before)
        after = jnp.where(lane == LANES - 1, hi, after)
    return part[32:64] + before + after


def fine_kernel(x_ref, t1, w0, wf, acc_out, f0):
    lane = lanes()
    zero = jnp.zeros((32, LANES), BF16)
    for i in range(10):
        f0[i, 0] = zero
        f0[i, 9] = zero
        f0[0, i] = zero
        f0[9, i] = zero
    f0[1:9, 1:9] = x_ref[...]
    low = jnp.zeros((32, LANES), F32)
    high = jnp.zeros((32, LANES), F32)
    for i in range(4):
        for j in range(4):
            value = t1[i, j].astype(F32)
            for sx in range(2):
                spot = 12 * (2 * i + sx + 1) + 2 * j + 1
                here = (lane >= spot) & (lane < spot + 2)
                low = jnp.where(here, rolled(value, spot - 124 - 2 * sx), low)
                high = jnp.where(here, rolled(value, spot - 68 - 2 * sx), high)

    def columns(value, dz):
        near = [rolled(value, -12 * dx - dy).astype(BF16) for dx in (-1, 0, 1) for dy in (-1, 0, 1)]
        return weighted(block(w0, dz), jnp.concatenate(near, axis=0))

    low, high = columns(low, 0), columns(high, 2)
    for x in range(8):
        for y in range(0, 8, GROUP):
            ys = range(y, y + GROUP)
            middle = jnp.concatenate([x_ref[x, k] for k in ys], axis=1)
            value = dot(wf[...], jnp.concatenate([around(f0, x, ys), middle], axis=0))
            for n, k in enumerate(ys):
                spot = 12 * (x + 1) + k + 1
                acc_out[x, k] = shifted(value, n, rolled(low, -spot), rolled(high, 127 - spot))


def own_rows_kernel(
    flags, t1, t2, t3, xr_lo, xr_hi, xr_lo2, xr_hi2, w0, wf1, wf2, wf3,
    edge_out, a1_out, a2_out, a3_out, ex, f1, f2, f3,
):
    x_lo, x_hi, x_lo2, x_hi2 = flags[0:1], flags[1:2], flags[6:7], flags[7:8]
    zero = jnp.zeros((32, LANES), BF16)
    for ref, size in ((f1, 6), (f2, 4), (f3, 3)):
        for i in range(size + 2):
            for j in (0, 1, size, size + 1):
                ref[i, j] = zero
    for side in range(2):
        for j in (0, 9):
            ex[side, j] = jnp.zeros((96, LANES), BF16)
    for k in range(8):
        s = k % 2
        column = kept(x_lo, xr_lo[8 + 4 + k // 2]).astype(F32)
        spread(ex, 0, 1 + k, kept(x_lo, xr_lo[k]), 0, rolled(column, 2 - s), rolled(column, 57 - s))
        column = kept(x_hi, xr_hi[8 + k // 2]).astype(F32)
        spread(ex, 1, 1 + k, kept(x_hi, xr_hi[k]), 0, rolled(column, 4 - s), rolled(column, 59 - s))

    def back(value):
        return rolled(value.astype(F32), -72).astype(BF16)

    for k in range(4):
        for i in range(2):
            f1[i, 2 + k] = kept(x_lo, xr_lo[8 + 4 * i + k])
            f1[6 + i, 2 + k] = kept(x_hi, xr_hi[8 + 4 * i + k])
        for i in range(4):
            f1[2 + i, 2 + k] = t1[i, k]
    for i in range(2):
        for k in range(2):
            f2[i, 2 + k] = back(kept(x_lo, xr_lo[8 + 2 * i + k]))
            f2[2 + i, 2 + k] = t2[i, k]
            f2[4 + i, 2 + k] = back(kept(x_hi, xr_hi[8 + 2 * i + k]))
    f3[0, 2] = kept(x_lo2, xr_lo2[...])
    f3[1, 2] = back(kept(x_lo, xr_lo[12]))
    f3[2, 2] = t3[...]
    f3[3, 2] = back(kept(x_hi, xr_hi[12]))
    f3[4, 2] = kept(x_hi2, xr_hi2[...])

    for side, dx in ((0, 0), (1, 2)):
        weight = w0[288 * dx : 288 * dx + 288]
        for y in range(0, 8, 2):
            value = jnp.concatenate(
                [ex[side, y : y + 3].reshape(288, LANES), ex[side, y + 1 : y + 4].reshape(288, LANES)], axis=1
            )
            value = weighted(weight, value)
            edge_out[side, y] = value[:, :LANES]
            edge_out[side, y + 1] = value[:, LANES:]
    for ref, w, out, size in ((f3, wf3, a3_out, 3), (f2, wf2, a2_out, 4), (f1, wf1, a1_out, 6)):
        for i in range(size):
            value = dot(w[...], around(ref, i, range(size)))
            for j in range(size):
                out[i, j] = shifted(value, j)


def final_kernel(
    flags, acc, edge_x, a1, a2, a3, yn_lo, yn_hi, yr_lo, yr_hi, yr_two,
    w0, wf1, wf2, wf3, up, up0, out_hbm, ey, edge, f1, f2, f3, v3, v2, v1, q1, rows, out, sems,
):
    x_lo, x_hi, y_lo, y_hi, z_lo, z_hi = (flags[i : i + 1] for i in range(6))
    y_lo2, y_hi2 = flags[8:9], flags[9:10]
    lane = lanes()

    zero = jnp.zeros((32, LANES), BF16)
    for ref, size in ((f1, 6), (f2, 4), (f3, 3)):
        for i in range(size + 2):
            for j in range(2, size):
                ref[i, j] = zero

    def back(flag, value, shift):
        return rolled(kept(flag, value).astype(F32), -shift).astype(BF16)

    for i in range(5):
        f3[i, 0] = back(y_lo2, yr_two[...], 20 * i)
        f3[i, 1] = back(y_lo, yr_lo[10], 20 * i)
        f3[i, 3] = back(y_hi, yr_hi[10], 20 * i)
        f3[i, 4] = back(y_hi2, yr_two[...], 20 * i)
    for i in range(6):
        for k in range(2):
            f2[i, k] = back(y_lo, quarter_tile(yn_lo, yr_lo, i, k), 72)
            f2[i, 4 + k] = back(y_hi, quarter_tile(yn_hi, yr_hi, i, k), 72)
    for i in range(8):
        for k in range(2):
            f1[i, k] = kept(y_lo, half_tile(yn_lo, yr_lo, i, k))
            f1[i, 6 + k] = kept(y_hi, half_tile(yn_hi, yr_hi, i, k))
    for i in range(10):
        sx = (i + 1) % 2
        coarse = (i + 1) // 2 + 1
        for side, near, far, flag, row, s in (
            (0, yn_lo, yr_lo, y_lo, 1, 2 * sx + 1), (1, yn_hi, yr_hi, y_hi, 0, 2 * sx)
        ):
            column = kept(flag, half_tile(near, far, coarse, row)).astype(F32)
            spread(ey, side, i, kept(flag, fine_row(near, far, i)), 0, rolled(column, 4 - s), rolled(column, 59 - s))
    for side, dy in ((0, 0), (1, 2)):
        weight = jnp.concatenate([w0[96 * (3 * dx + dy) : 96 * (3 * dx + dy) + 96] for dx in range(3)], axis=0)
        for x in range(0, 8, 2):
            value = jnp.concatenate(
                [ey[side, x : x + 3].reshape(288, LANES), ey[side, x + 1 : x + 4].reshape(288, LANES)], axis=1
            )
            value = weighted(weight, value)
            edge[side, x] = value[:, :LANES]
            edge[side, x + 1] = value[:, LANES:]

    def along(before, centre, after):
        return [0.75 * centre + 0.25 * before, 0.75 * centre + 0.25 * after]

    def limits(count):
        spot = lax.broadcasted_iota(jnp.int32, (1, LANES), 1)
        inside = jnp.where((spot >= 1) & (spot <= count + 2), 1.0, 0.0)
        return jnp.where(spot == 1, z_lo, jnp.where(spot == count + 2, z_hi, inside))

    def cell_flag(position, last, lo, hi):
        return lo if position == 0 else hi if position == last else None

    def prolonged(ref, count):
        wide = dot(ref[...].reshape(count * count * 32, LANES), up[...]).reshape(count, count, 32, LANES)

        def refined(cells):
            out = []
            for k in range(2 * count - 2):
                cell = k - 1
                centre = cell // 2 + 1
                other = centre - 1 if cell % 2 == 0 else centre + 1
                out.append(0.75 * cells[centre] + 0.25 * cells[other])
            return out

        by_x = refined([wide[i] for i in range(count)])
        return [refined([row[j] for j in range(count)]) for row in by_x]

    def level(ref, w_ref, own, v_ref, size, cells, above):
        keep = limits(cells)
        touched = [j for j in range(size) if j < 2 or j >= size - 2]
        for x in range(size):
            value = dot(w_ref[...], around(ref, x, touched))
            for j in range(size):
                part = own[x, j]
                if j in touched:
                    part = part + shifted(value, touched.index(j))
                if above is not None:
                    part = part + above[x][j]
                good = keep
                for flag in (cell_flag(x, size - 1, x_lo, x_hi), cell_flag(j, size - 1, y_lo, y_hi)):
                    if flag is not None:
                        good = good * flag
                v_ref[x, j] = (part * good).astype(BF16)

    level(f3, wf3, a3, v3, 3, 16, None)
    level(f2, wf2, a2, v2, 4, 32, prolonged(v3, 3))
    level(f1, wf1, a1, v1, 6, 64, prolonged(v2, 4))
    for i in range(6):
        q1[i] = dot(v1[i].reshape(6 * 32, LANES), up0[...]).reshape(6, 32, LANES)

    copies = []
    for x in range(8):
        c, part = x // 2, x % 2
        row = 0.75 * q1[c + 1] + 0.25 * q1[c + 2 * part]
        for y in range(0, 8, 2):
            centre = y // 2 + 1
            for n, extra in enumerate(along(row[centre - 1], row[centre], row[centre + 1])):
                total = acc[x, y + n] + extra
                if y + n == 0:
                    total = total + edge[0, x]
                if y + n == 7:
                    total = total + edge[1, x]
                if x == 0:
                    total = total + edge_x[0, y + n]
                if x == 7:
                    total = total + edge_x[1, y + n]
                rows[x, pl.ds(y + n, 32, stride=8), :] = jax.nn.gelu(total, approximate=True)
        out[x] = rows[x].reshape(32, 8, LANES).astype(BF16)
        copies.append(pltpu.make_async_copy(out.at[x], out_hbm.at[:, x], sems.at[x]))
        copies[-1].start()
    for copy in copies:
        copy.wait()


def turned(value, axis, step):
    count = lax.axis_size(axis)
    return lax.ppermute(value, axis, [(i, (i + step) % count) for i in range(count)])


def on_device(field, mixing, kernel_fine, kernel_half, kernel_quarter, kernel_eighth):
    gx, gy, gz = (lax.axis_index(a) for a in ("gx", "gy", "gz"))
    nx, ny, nz = (lax.axis_size(a) for a in ("gx", "gy", "gz"))
    slot = lax.broadcasted_iota(jnp.int32, (16, LANES), 0)
    place = jnp.where((slot < 2) | (slot == 6) | (slot == 7), gx, jnp.where((slot == 4) | (slot == 5), gz, gy))
    side = slot & 1
    width = jnp.where(slot < 6, 1, 2)
    count = jnp.where((slot < 2) | (slot == 6) | (slot == 7), nx, jnp.where((slot == 4) | (slot == 5), nz, ny))
    flags = jnp.where(side == 0, place >= width, place < count - width).astype(F32)
    up, up0 = (jnp.asarray(m) for m in tables())
    tile = (32, LANES)

    (table,) = call(restrictions, [(512, 640)], [], flops=1 << 26)
    x_own, t1, t2, t3, msg = call(
        restrict_kernel,
        [(8, 8) + tile, (4, 4) + tile, (2, 2) + tile, tile, (2,) + tile],
        [field, table],
        [pltpu.VMEM((2048, LANES), F32)],
    )
    flat = [k.reshape(864, 32) for k in (kernel_fine, kernel_half, kernel_quarter, kernel_eighth)]
    mixing, *flat, t3 = lax.optimization_barrier((mixing, *flat, t3))
    wf = call(weights_kernel, [(96, 320)] + [(96, 288)] * 3, [*flat, mixing], flops=1 << 28)
    from_hi = turned(msg[0], "gz", -1)
    from_lo = turned(msg[1], "gz", 1)
    from_lo, *wf = lax.optimization_barrier((from_lo, *wf))
    t1, t2, t3, x_msg_lo, x_msg_hi, y_near_lo, y_near_hi = call(
        depth_kernel,
        [(4, 4) + tile, (2, 2) + tile, tile] + [(16,) + tile] * 4,
        [flags, x_own, t1, t2, t3, from_lo, from_hi],
    )
    xr_hi = turned(x_msg_lo, "gx", -1)
    xr_lo = turned(x_msg_hi, "gx", 1)
    xr_hi2 = turned(t3, "gx", -2)
    xr_lo2 = turned(t3, "gx", 2)
    yn_hi = turned(y_near_lo, "gy", -1)
    yn_lo = turned(y_near_hi, "gy", 1)
    y_msg_lo, y_msg_hi, two = call(
        width_kernel,
        [(11,) + tile, (11,) + tile, tile],
        [flags, t3, xr_lo, xr_hi, xr_lo2, xr_hi2],
    )
    yr_hi = turned(y_msg_lo, "gy", -1)
    yr_lo = turned(y_msg_hi, "gy", 1)
    assert ny == 4
    yr_two = turned(two, "gy", 2)
    (acc,) = call(
        fine_kernel,
        [(8, 8) + tile],
        [x_own, t1, flat[0], wf[0]],
        [pltpu.VMEM((10, 10) + tile, BF16)],
        kind=F32,
        flops=1 << 30,
    )
    edge_x, a1, a2, a3 = call(
        own_rows_kernel,
        [(2, 8) + tile, (6, 6) + tile, (4, 4) + tile, (3, 3) + tile],
        [flags, t1, t2, t3, xr_lo, xr_hi, xr_lo2, xr_hi2, flat[0], *wf[1:]],
        [
            pltpu.VMEM((2, 10, 96, LANES), BF16),
            pltpu.VMEM((8, 8) + tile, BF16),
            pltpu.VMEM((6, 6) + tile, BF16),
            pltpu.VMEM((5, 5) + tile, BF16),
        ],
        kind=F32,
        flops=1 << 30,
    )
    (out,) = call(
        final_kernel,
        [(32, 8, 8, LANES)],
        [flags, acc, edge_x, a1, a2, a3, yn_lo, yn_hi, yr_lo, yr_hi, yr_two, flat[0], *wf[1:], up, up0],
        [
            pltpu.VMEM((2, 10, 96, LANES), BF16),
            pltpu.VMEM((2, 8) + tile, F32),
            pltpu.VMEM((8, 8) + tile, BF16),
            pltpu.VMEM((6, 6) + tile, BF16),
            pltpu.VMEM((5, 5) + tile, BF16),
            pltpu.VMEM((3, 3) + tile, BF16),
            pltpu.VMEM((4, 4) + tile, BF16),
            pltpu.VMEM((6, 6) + tile, BF16),
            pltpu.VMEM((6, 6) + tile, F32),
            pltpu.VMEM((8, 256, LANES), F32),
            pltpu.VMEM((8, 32, 8, LANES), BF16),
            pltpu.SemaphoreType.DMA((8,)),
        ],
        out_space=pl.ANY,
    )
    return out


def solution(mesh):
    placed = (P(None, "gx", "gy", "gz"), P(), P(), P(), P(), P())

    return jax.shard_map(on_device, mesh=mesh, in_specs=placed, out_specs=P(None, "gx", "gy", "gz"), check_vma=False)
```
